16 devices in a mesh: dp: 2 (over z), col: 2 (over y), fsdp: 4 (over x, core).
Axes of the slice: x: 2, y: 2, z: 2, core: 2. Of those that a mesh axis runs over, the one named last changes fastest.
Arguments:
- x_act: bfloat16 [65536, 960], P(('dp', 'col', 'fsdp'))
- dy_out: bfloat16 [65536, 960], P(('dp', 'col', 'fsdp'))
- w_gate: bfloat16 [960, 2560], P(None, ('col', 'fsdp'))
- w_up: bfloat16 [960, 2560], P(None, ('col', 'fsdp'))
- w_down: bfloat16 [2560, 960], P(('col', 'fsdp'))
- v_gate: bfloat16 [960, 2560], P(None, ('col', 'fsdp'))
- v_up: bfloat16 [960, 2560], P(None, ('col', 'fsdp'))
- v_down: bfloat16 [2560, 960], P(('col', 'fsdp'))
- g_next: float32 [16, 3, 960, 2560], P(('dp', 'col', 'fsdp'))
Outputs:
- output 1: bfloat16 [65536, 960], P(('dp', 'col', 'fsdp'))
- output 2: float32 [3, 960, 2560], P(None, None, ('col', 'fsdp'))
- output 3: float32 [16, 3, 960, 2560], P(('dp', 'col', 'fsdp'))
- output 4: bfloat16 [960, 2560], replicated
- output 5: bfloat16 [960, 2560], replicated
- output 6: bfloat16 [2560, 960], replicated
All inputs are finite; a program needn't handle non-finite values.
Results may differ from the reference program's by a relative error of at most 0.0105823.
Values are sent between devices in bfloat16 or wider.
A program may use at most 1 GiB of HBM per device.

```python
import jax
import jax.numpy as jnp
from jax import lax

D_MODEL = 960
D_FF = 2560
TOKENS_DEV = 4096
N_DEVICES = 16


def draw_normal(key, shape, scaling):
    return jax.random.normal(key, shape, jnp.float32) * scaling


def setup_inputs(seed: int = 0) -> dict:
    keys = jax.random.split(jax.random.key(seed), 9)
    all_rows = N_DEVICES * TOKENS_DEV
    model_scale = D_MODEL ** -0.5
    hidden_scale = D_FF ** -0.5
    return {
        'x_act': draw_normal(keys[0], (all_rows, D_MODEL), 1.0).astype(jnp.bfloat16),
        'dy_out': draw_normal(keys[1], (all_rows, D_MODEL), 1.0).astype(jnp.bfloat16),
        'w_gate': draw_normal(keys[2], (D_MODEL, D_FF), model_scale).astype(jnp.bfloat16),
        'w_up': draw_normal(keys[3], (D_MODEL, D_FF), model_scale).astype(jnp.bfloat16),
        'w_down': draw_normal(keys[4], (D_FF, D_MODEL), hidden_scale).astype(jnp.bfloat16),
        'v_gate': draw_normal(keys[5], (D_MODEL, D_FF), model_scale).astype(jnp.bfloat16),
        'v_up': draw_normal(keys[6], (D_MODEL, D_FF), model_scale).astype(jnp.bfloat16),
        'v_down': draw_normal(keys[7], (D_FF, D_MODEL), hidden_scale).astype(jnp.bfloat16),
        'g_next': draw_normal(keys[8], (N_DEVICES, 3, D_MODEL, D_FF), 1.0),
    }


def reference(x_act, dy_out, w_gate, w_up, w_down, v_gate, v_up, v_down, g_next):
    x_dev = x_act.reshape(N_DEVICES, TOKENS_DEV, D_MODEL)
    dy_dev = dy_out.reshape(N_DEVICES, TOKENS_DEV, D_MODEL)

    def one_device(operands):
        x_loc, dy_loc = operands
        pre_gate = jnp.dot(x_loc, w_gate, preferred_element_type=jnp.float32)
        pre_up = jnp.dot(x_loc, w_up, preferred_element_type=jnp.float32)
        sig_gate = jax.nn.sigmoid(pre_gate)
        act_gate = pre_gate * sig_gate
        hidden = (act_gate * pre_up).astype(jnp.bfloat16)
        d_hidden = jnp.dot(dy_loc, w_down.T, preferred_element_type=jnp.float32)
        d_gate = (d_hidden * pre_up * sig_gate * (1.0 + pre_gate * (1.0 - sig_gate))).astype(jnp.bfloat16)
        d_up = (d_hidden * act_gate).astype(jnp.bfloat16)
        dx_loc = (jnp.dot(d_gate, w_gate.T, preferred_element_type=jnp.float32)
                  + jnp.dot(d_up, w_up.T, preferred_element_type=jnp.float32)).astype(jnp.bfloat16)
        grad_gate = jnp.dot(x_loc.T, d_gate, preferred_element_type=jnp.float32)
        grad_up = jnp.dot(x_loc.T, d_up, preferred_element_type=jnp.float32)
        grad_down_t = jnp.dot(dy_loc.T, hidden, preferred_element_type=jnp.float32)
        return dx_loc, jnp.stack([grad_gate, grad_up, grad_down_t])

    dx_dev, dw_local = lax.map(one_device, (x_dev, dy_dev))
    dx_in = dx_dev.reshape(N_DEVICES * TOKENS_DEV, D_MODEL)
    dw_next = jnp.sum(g_next.astype(jnp.bfloat16).astype(jnp.float32), axis=0)
    return dx_in, dw_next, dw_local, v_gate, v_up, v_down
```

```python
import jax
import jax.numpy as jnp
from jax import lax
from jax.experimental import pallas as pl
from jax.experimental.pallas import tpu as pltpu
from jax.sharding import PartitionSpec as P

ALL_AXES = ('dp', 'col', 'fsdp')
FSDP_AXES = ('col', 'fsdp')
MESH = pl.DeviceIdType.MESH
BF16 = jnp.bfloat16
F32 = jnp.float32

D = 960
F = 2560
T = 4096
SH = F // 8
CH = F // 4
TM = 512
NI = T // TM
NC = 4
SUB = 320

NN = (((1,), (0,)), ((), ()))
NT = (((1,), (1,)), ((), ()))


def dotf(a, b, dims):
    return lax.dot_general(a, b, dims, preferred_element_type=F32)


def step_kernel(x_hbm, dy_hbm, w1_hbm, w3_hbm, w2_hbm, v1_hbm, v3_hbm, v2_hbm,
                h3_hbm, dx_hbm, v_out,
                x_v, dy_v, acc, w_v, wt, hbuf,
                lsem, hsem, xsem, send, recv):
    z = lax.axis_index('dp')
    y = lax.axis_index('col')
    fs = lax.axis_index('fsdp')
    x = fs // 2
    c = fs % 2
    partner = {'fsdp': x * 2 + (1 - c)}
    xnbr = {'fsdp': (1 - x) * 2 + c}
    ynbr = {'col': 1 - y}
    znbr = {'dp': 1 - z}
    q_own = y * 2 + x
    q_x = y * 2 + (1 - x)
    q_y = (1 - y) * 2 + x
    q_d = (1 - y) * 2 + (1 - x)

    def remote(src, dst, dev, k):
        return pltpu.make_async_remote_copy(src, dst, send.at[k], recv.at[k],
                                            device_id=dev, device_id_type=MESH)

    class Gather:
        def __init__(self, base, srcs, dst, zsplit):
            self.base, self.srcs, self.dst, self.zsplit = base, srcs, dst, zsplit
            self.lo = z * 160 if zsplit else 0
            self.n = 160 if zsplit else 320

        def blk(self, a, q, lo, n):
            return self.dst.at[a, pl.ds(pl.multiple_of(q * CH + c * SH + lo, 16), n), :]

        def copy(self, kind, a):
            k = self.base + 3 * ('x0', 'x1', 'y0', 'y1', 'xf', 'yf', 'zx', 'zy', 'zd', 'dx', 'dy', 'dd').index(kind) + a
            h = self.n // 2
            if kind in ('x0', 'x1', 'y0', 'y1'):
                lo = self.lo + (h if kind[1] == '1' else 0)
                return remote(self.srcs[a].at[pl.ds(pl.multiple_of(lo, 16), h), :], self.blk(a, q_own, lo, h),
                              xnbr if kind[0] == 'x' else ynbr, k)
            if kind == 'yf':
                return remote(self.blk(a, q_x, self.lo, h), self.blk(a, q_x, self.lo, h), ynbr, k)
            if kind == 'xf':
                return remote(self.blk(a, q_y, self.lo + h, h), self.blk(a, q_y, self.lo + h, h), xnbr, k)
            q = {'x': q_x, 'y': q_y, 'd': q_d}[kind[1]]
            if kind[0] == 'z':
                return remote(self.blk(a, q, self.lo, self.n), self.blk(a, q, self.lo, self.n), znbr, k)
            return remote(self.blk(a, q, 0, SH), self.blk(a, q, 0, SH), partner, k)

        def start(self, *kinds):
            for kind in kinds:
                for a in range(3):
                    self.copy(kind, a).start()

        def recv(self, *kinds):
            for kind in kinds:
                for a in range(3):
                    self.copy(kind, a).wait_recv()

        def sent(self):
            for kind in ('x0', 'x1', 'y0', 'y1', 'xf', 'yf', 'dx', 'dy', 'dd') + (
                    ('zx', 'zy', 'zd') if self.zsplit else ()):
                for a in range(3):
                    self.copy(kind, a).wait_send()

    w_hbm = (w1_hbm, w3_hbm, w2_hbm)
    v_hbm = (v1_hbm, v3_hbm, v2_hbm)
    gw = Gather(0, w_hbm, w_v, True)
    gv = Gather(36, v_hbm, v_out, False)

    def local(src, dst, k):
        return pltpu.make_async_copy(src, dst, lsem.at[k])

    pw = [remote(w_hbm[a], gw.blk(a, q_own, 0, SH), partner, 72 + a) for a in range(3)]
    pv = [remote(v_hbm[a], gv.blk(a, q_own, 0, SH), partner, 75 + a) for a in range(3)]
    lw = [local(w_hbm[a], gw.blk(a, q_own, 0, SH), a) for a in range(3)]
    lv = [local(v_hbm[a], gv.blk(a, q_own, 0, SH), 3 + a) for a in range(3)]
    lx = [local(x_hbm, x_v, 6), local(dy_hbm, dy_v, 7)]

    for cp in lw + lx:
        cp.start()
    bar = pltpu.get_barrier_semaphore()
    for dev in (partner, xnbr, ynbr, znbr):
        pl.semaphore_signal(bar, inc=1, device_id=dev, device_id_type=MESH)
    pl.semaphore_wait(bar, 4)
    for cp in pw:
        cp.start()
    gw.start('x0', 'y1', 'x1', 'y0')

    def zero(r, _):
        acc[pl.ds(pl.multiple_of(r * 16, 16), 16), :] = jnp.zeros((16, T), F32)
        return 0
    lax.fori_loop(0, D // 16, zero, 0)

    for cp in lw + lx:
        cp.wait()
    for cp in pw:
        cp.wait_recv()

    def body(n, _):
        j = n // NI
        i = n % NI

        def at(k):
            return pl.when(n == k)

        @at(3)
        def _():
            gw.recv('x0', 'x1')
            gw.start('zx', 'yf')
            gw.recv('y0', 'y1')
            gw.start('xf', 'zy')

        @at(8)
        def _():
            gw.recv('zx')
            gw.start('dx')
            gw.recv('dx')

        @at(10)
        def _():
            for cp in lv + pv:
                cp.start()
            gv.start('x0', 'y1', 'x1', 'y0')
            gw.recv('xf', 'yf')
            gw.start('zd')

        @at(14)
        def _():
            gw.recv('zy')
            gw.start('dy')

        @at(16)
        def _():
            gw.recv('dy')

        @at(20)
        def _():
            gw.recv('zd')
            gw.start('dd')

        @at(22)
        def _():
            gv.recv('x0')
            gv.start('yf')
            gv.recv('y1')
            gv.start('xf')

        @at(24)
        def _():
            gw.recv('dd')

        @at(26)
        def _():
            gv.recv('x1', 'y0')
            gv.start('dx', 'dy')

        q = jnp.where(j == 0, q_own, jnp.where(j == 1, q_x, jnp.where(j == 2, q_y, q_d)))
        base = pl.multiple_of(q * CH, CH)

        @pl.when(i == 0)
        def _():
            def tr(r, _):
                src = pl.ds(pl.multiple_of(base + r * 128, 128), 128)
                for a in range(2):
                    wt[:, pl.ds(pl.multiple_of(a * CH + r * 128, 128), 128)] = w_v[a, src, :].T
                return 0
            lax.fori_loop(0, CH // 128, tr, 0)

        cols = pl.ds(pl.multiple_of(i * TM, TM), TM)
        slot = n % 2

        def hcopies(slot):
            return [pltpu.make_async_copy(hbuf.at[slot, pl.ds(a * CH, CH), :],
                                          h3_hbm.at[a, pl.ds(base, CH), cols], hsem.at[slot, a]) for a in range(3)]

        @pl.when(n >= 2)
        def _():
            for cp in hcopies(slot):
                cp.wait()

        for r in range(CH // SUB):
            src = pl.ds(pl.multiple_of(base + r * SUB, 16), SUB)
            a = dotf(w_v[0, src, :], x_v[:, cols], NN)
            b = dotf(w_v[1, src, :], x_v[:, cols], NN)
            dh = dotf(w_v[2, src, :], dy_v[:, cols], NN)
            s = 1.0 / (1.0 + jnp.exp(-a))
            act = a * s
            hbuf[slot, r * SUB:(r + 1) * SUB, :] = (dh * b * s * (1.0 + a * (1.0 - s))).astype(BF16)
            hbuf[slot, CH + r * SUB:CH + (r + 1) * SUB, :] = (dh * act).astype(BF16)
            hbuf[slot, 2 * CH + r * SUB:2 * CH + (r + 1) * SUB, :] = (act * b).astype(BF16)
        for cp in hcopies(slot):
            cp.start()
        acc[:, cols] += dotf(wt[...], hbuf[slot, 0:2 * CH, :], NN)

        @pl.when(j == NC - 1)
        def _():
            x_v[:, cols] = acc[:, cols].astype(BF16)
            pltpu.make_async_copy(x_v.at[:, cols], dx_hbm.at[:, cols], xsem).start()
        return 0

    lax.fori_loop(0, NC * NI, body, 0)

    gv.recv('xf', 'yf')
    gv.start('dd')
    for slot in range(2):
        for a in range(3):
            pltpu.make_async_copy(hbuf.at[slot, pl.ds(a * CH, CH), :],
                                  h3_hbm.at[a, pl.ds(0, CH), pl.ds(0, TM)], hsem.at[slot, a]).wait()
    pltpu.make_async_copy(x_v, dx_hbm, xsem).wait()
    for cp in lv:
        cp.wait()
    for cp in pv:
        cp.wait_recv()
    gv.recv('dx', 'dy', 'dd')
    for cp in pw + pv:
        cp.wait_send()
    gw.sent()
    gv.sent()


def run_step(*args):
    hbm = pl.BlockSpec(memory_space=pltpu.MemorySpace.HBM)
    return pl.pallas_call(
        step_kernel,
        out_shape=(jax.ShapeDtypeStruct((3, F, T), BF16), jax.ShapeDtypeStruct((D, T), BF16),
                   jax.ShapeDtypeStruct((3, F, D), BF16)),
        in_specs=[hbm] * 8,
        out_specs=(hbm,) * 3,
        scratch_shapes=[
            pltpu.VMEM((D, T), BF16), pltpu.VMEM((D, T), BF16), pltpu.VMEM((D, T), F32),
            pltpu.VMEM((3, F, D), BF16), pltpu.VMEM((D, 2 * CH), BF16),
            pltpu.VMEM((2, 3 * CH, TM), BF16),
            pltpu.SemaphoreType.DMA((8,)), pltpu.SemaphoreType.DMA((2, 3)), pltpu.SemaphoreType.DMA,
            pltpu.SemaphoreType.DMA((78,)), pltpu.SemaphoreType.DMA((78,)),
        ],
        compiler_params=pltpu.CompilerParams(collective_id=0, has_side_effects=True,
                                             vmem_limit_bytes=66_000_000),
        cost_estimate=pl.CostEstimate(flops=10 * T * D * F, bytes_accessed=120_000_000, transcendentals=T * F),
    )(*args)


def grad_kernel(x_ref, dy_ref, h3_ref, dx_ref, v_ref,
                dw_ref, dxo_ref, v1o_ref, v3o_ref, v2o_ref):
    s = pl.program_id(0)
    for k, (lhs, vo) in enumerate(((x_ref, v1o_ref), (x_ref, v3o_ref), (dy_ref, v2o_ref))):
        @pl.when(s // 5 == k)
        def _():
            dxo_ref[...] = dx_ref[...]
            vo[...] = v_ref[0].T
            dw_ref[0, 0] = dotf(lhs[...], h3_ref[0], NT)


def run_grad(x, dy, h3, dx, v):
    one = pl.Buffered(1)
    whole = pl.BlockSpec((D, T), lambda s: (0, 0), pipeline_mode=one)
    dxs = pl.BlockSpec((D // 15, T), lambda s: (s, 0))

    def vspec(k):
        return pl.BlockSpec((D, 512), lambda s: (0, jnp.clip(s - 5 * k, 0, 4)))
    return pl.pallas_call(
        grad_kernel,
        grid=(15,),
        out_shape=(jax.ShapeDtypeStruct((1, 3, D, F), F32), jax.ShapeDtypeStruct((D, T), BF16),
                   jax.ShapeDtypeStruct((D, F), BF16), jax.ShapeDtypeStruct((D, F), BF16),
                   jax.ShapeDtypeStruct((D, F), BF16)),
        in_specs=[whole, whole, pl.BlockSpec((1, 512, T), lambda s: (s // 5, s % 5, 0)), dxs,
                  pl.BlockSpec((1, 512, D), lambda s: (s // 5, s % 5, 0))],
        out_specs=(pl.BlockSpec((1, 1, D, 512), lambda s: (0, s // 5, 0, s % 5)), dxs, vspec(0), vspec(1), vspec(2)),
        compiler_params=pltpu.CompilerParams(vmem_limit_bytes=64_000_000),
        cost_estimate=pl.CostEstimate(flops=6 * T * D * F, bytes_accessed=150_000_000, transcendentals=0),
    )(x, dy, h3, dx, v)


def solution(mesh):
    def device_step(x, dy, w1, w3, w2, v1, v3, v2, g_next):
        part = lax.psum_scatter(g_next[0].astype(BF16), FSDP_AXES, scatter_dimension=2, tiled=True)
        xt, dyt = x.T, dy.T
        h3, dx, v = run_step(xt, dyt, w1.T, w3.T, w2, v1.T, v3.T, v2)
        other = lax.ppermute(part, 'dp', [(0, 1), (1, 0)])
        dw, dxo, v1o, v3o, v2o = run_grad(xt, dyt, h3, dx, v)
        grad_next = part.astype(F32) + other.astype(F32)
        return dxo.T, grad_next, dw, v1o, v3o, v2o.T

    row_spec = P(ALL_AXES, None)
    col_shard = P(None, FSDP_AXES)
    row_shard = P(FSDP_AXES, None)
    dev_spec = P(ALL_AXES, None, None, None)
    return jax.shard_map(
        device_step, mesh=mesh,
        in_specs=(row_spec, row_spec, col_shard, col_shard, row_shard, col_shard, col_shard, row_shard, dev_spec),
        out_specs=(row_spec, P(None, None, FSDP_AXES), dev_spec, P(), P(), P()),
        check_vma=False)
```

```python
import jax
import jax.numpy as jnp
from jax import lax
from jax.experimental import pallas as pl
from jax.experimental.pallas import tpu as pltpu
from jax.sharding import PartitionSpec as P

ALL_AXES = ('dp', 'col', 'fsdp')
FSDP_AXES = ('col', 'fsdp')
MESH = pl.DeviceIdType.MESH
BF16 = jnp.bfloat16
F32 = jnp.float32

D = 960
F = 2560
T = 4096
SH = F // 8
CH = F // 4
TM = 512
NI = T // TM
NC = 4
SUB = 320
HR = D // 2
QR = HR // 2
S2 = 3
G_AT = (13, 16, 18, 20, 23, 25)

NN = (((1,), (0,)), ((), ()))
NT = (((1,), (1,)), ((), ()))


def dotf(a, b, dims):
    return lax.dot_general(a, b, dims, preferred_element_type=F32)


def step_kernel(x_hbm, dy_hbm, w1_hbm, w3_hbm, w2_hbm, v1_hbm, v3_hbm, v2_hbm, g_hbm,
                h3_hbm, dx_hbm, v_out, sg, r1, pp, rx, ry, rx2, ry2, sx, sy,
                x_v, dy_v, acc, w_v, wt, hbuf, gin1, gout1, gin2, rin, gout2, ab, ob,
                lsem, hsem, xsem, send, recv, g1l, g1s, g1r, g2l, gps, gpr, abl, obs, gms, gmr, zs, zr):
    z = lax.axis_index('dp')
    y = lax.axis_index('col')
    fs = lax.axis_index('fsdp')
    x = fs // 2
    c = fs % 2
    partner = {'fsdp': x * 2 + (1 - c)}
    xnbr = {'fsdp': (1 - x) * 2 + c}
    ynbr = {'col': 1 - y}
    znbr = {'dp': 1 - z}
    q_own = y * 2 + x
    q_x = y * 2 + (1 - x)
    q_y = (1 - y) * 2 + x
    q_d = (1 - y) * 2 + (1 - x)

    def rdma(src, dst, ssem, rsem, dev):
        return pltpu.make_async_remote_copy(src, dst, ssem, rsem, device_id=dev, device_id_type=MESH)

    def remote(src, dst, dev, k):
        return rdma(src, dst, send.at[k], recv.at[k], dev)

    class Gather:
        KINDS = ('x0', 'x1', 'y0', 'y1', 'xf', 'yf', 'dx', 'dy', 'dd', 'zx0', 'zx1', 'zy0', 'zy1', 'zd0', 'zd1')

        def __init__(self, base, srcs, dst, arrays, zsplit):
            self.base, self.srcs, self.dst, self.arrays, self.zsplit = base, srcs, dst, arrays, zsplit
            self.lo = z * 160 if zsplit else 0
            self.n = 160 if zsplit else 320

        def blk(self, a, q, lo, n):
            return self.dst.at[a, pl.ds(pl.multiple_of(q * CH + c * SH + lo, 16), n), :]

        def copy(self, kind, a):
            k = self.base + len(self.arrays) * self.KINDS.index(kind) + self.arrays.index(a)
            h = self.n // 2
            if kind in ('x0', 'x1', 'y0', 'y1'):
                lo = self.lo + h * int(kind[1])
                return remote(self.srcs[a].at[pl.ds(pl.multiple_of(lo, 16), h), :], self.blk(a, q_own, lo, h),
                              xnbr if kind[0] == 'x' else ynbr, k)
            if kind == 'yf':
                return remote(self.blk(a, q_x, self.lo, h), self.blk(a, q_x, self.lo, h), ynbr, k)
            if kind == 'xf':
                return remote(self.blk(a, q_y, self.lo + h, h), self.blk(a, q_y, self.lo + h, h), xnbr, k)
            q = {'x': q_x, 'y': q_y, 'd': q_d}[kind[1]]
            if kind[0] == 'z':
                b = self.blk(a, q, self.lo + h * int(kind[2]), h)
                return remote(b, b, znbr, k)
            return remote(self.blk(a, q, 0, SH), self.blk(a, q, 0, SH), partner, k)

        def start(self, *kinds):
            for kind in kinds:
                for a in self.arrays:
                    self.copy(kind, a).start()

        def recv(self, *kinds):
            for kind in kinds:
                for a in self.arrays:
                    self.copy(kind, a).wait_recv()

        def sent(self):
            for kind in self.KINDS[:15 if self.zsplit else 9]:
                for a in self.arrays:
                    self.copy(kind, a).wait_send()

    w_hbm = (w1_hbm, w3_hbm, w2_hbm)
    v_hbm = (v1_hbm, v3_hbm, v2_hbm)
    gw = Gather(0, w_hbm, w_v, (0, 1, 2), True)
    gva = Gather(45, v_hbm, v_out, (0,), True)
    gvb = Gather(60, v_hbm, v_out, (1, 2), False)

    def local(src, dst, k):
        return pltpu.make_async_copy(src, dst, lsem.at[k])

    pw = [remote(w_hbm[a], gw.blk(a, q_own, 0, SH), partner, 78 + a) for a in range(3)]
    pv = [remote(v_hbm[a], gva.blk(a, q_own, 0, SH), partner, 81 + a) for a in range(3)]
    lw = [local(w_hbm[a], gw.blk(a, q_own, 0, SH), a) for a in range(3)]
    lv = [local(v_hbm[a], gva.blk(a, q_own, 0, SH), 3 + a) for a in range(3)]
    lx = [local(x_hbm, x_v, 6), local(dy_hbm, dy_v, 7)]

    def cols_of(q):
        return pl.ds(pl.multiple_of(q * CH, 128), CH)

    def unit(u):
        m = u % 4
        q = jnp.where(m == 0, q_d, jnp.where(m == 1, q_x, jnp.where(m == 2, q_y, q_own)))
        return u // 4, cols_of(q)

    def half(h):
        return pl.ds(pl.multiple_of(h * HR, 16), HR)

    def g1_load(u):
        k, cq = unit(u)
        return pltpu.make_async_copy(g_hbm.at[k, half(1 - c), cq], gin1, g1l)

    def g1_send(u):
        k, _ = unit(u)
        return rdma(gout1, r1.at[u], g1s, g1r.at[u], partner)

    def g2_loads(u):
        k, cq = unit(u)
        return (pltpu.make_async_copy(g_hbm.at[k, half(c), cq], gin2, g2l.at[0]),
                pltpu.make_async_copy(r1.at[u], rin, g2l.at[1]))

    def g2_out(u):
        return pltpu.make_async_copy(gout2, pp.at[u], g2l.at[2])

    def px(k, m):
        return rdma(pp.at[4 * k + m, pl.ds(0, QR), :], rx.at[k, m], gps.at[0, k, m], gpr.at[0, k, m], xnbr)

    def py(k, m):
        return rdma(pp.at[4 * k + 2 * m, pl.ds(QR, QR), :], ry.at[k, m], gps.at[1, k, m], gpr.at[1, k, m], ynbr)

    def g_stage1(u):
        @pl.when(u > 0)
        def _():
            g1_send(u - 1).wait_send()
        g1_load(u).wait()

        def cast(r, _):
            rows = pl.ds(pl.multiple_of(r * 48, 16), 48)
            gout1[rows, :] = gin1[rows, :].astype(BF16)
            return 0
        lax.fori_loop(0, HR // 48, cast, 0)
        g1_send(u).start()

        @pl.when(u < 11)
        def _():
            g1_load(u + 1).start()

    def g_sends(u):
        g2_out(u).wait()
        k = u // 4

        @pl.when(u % 4 == 0)
        def _():
            px(k, 0).start()
            py(k, 0).start()

        @pl.when(u % 4 == 1)
        def _():
            px(k, 1).start()

        @pl.when(u % 4 == 2)
        def _():
            py(k, 1).start()

    def g_stage2(u):
        for cp in g2_loads(u):
            cp.wait()

        def add(r, _):
            rows = pl.ds(pl.multiple_of(r * 48, 16), 48)
            gout2[rows, :] = (gin2[rows, :].astype(BF16).astype(F32) + rin[rows, :].astype(F32)).astype(BF16)
            return 0
        lax.fori_loop(0, HR // 48, add, 0)
        g2_out(u).start()

        @pl.when(u < 11)
        def _():
            g1_send(u + 1).wait_recv()
            for cp in g2_loads(u + 1):
                cp.start()

    def mid_sends(k):
        return (rdma(sy.at[k], ry2.at[k], gms.at[0, k], gmr.at[0, k], ynbr),
                rdma(sx.at[k], rx2.at[k], gms.at[1, k], gmr.at[1, k], xnbr))

    def ab_loads(k, fin):
        lo, hi = pl.ds(0, QR), pl.ds(QR, QR)
        if fin:
            srcs = (pp.at[4 * k + 3, lo, :], rx.at[k, 1], ry2.at[k], pp.at[4 * k + 3, hi, :], ry.at[k, 1], rx2.at[k])
        else:
            srcs = (pp.at[4 * k + 2, lo, :], rx.at[k, 0], pp.at[4 * k + 1, hi, :], ry.at[k, 0])
        return [pltpu.make_async_copy(s, ab.at[n], abl.at[n]) for n, s in enumerate(srcs)]

    def sg_half(s, k):
        return sg.at[s, k, half(c), :]

    def ob_outs(k, fin):
        if fin:
            dst = [sg.at[0, k, pl.ds(pl.multiple_of(c * HR + p * QR, 16), QR), :] for p in range(2)]
        else:
            dst = [sy.at[k], sx.at[k]]
        return [pltpu.make_async_copy(ob.at[p], dst[p], obs.at[p]) for p in range(2)]

    def z_sends(k):
        return (rdma(sg_half(0, k), sg_half(1, k), zs.at[0, k], zr.at[0, k], znbr),
                rdma(sg_half(0, k), sg_half(0, k), zs.at[1, k], zr.at[1, k], partner))

    def z_fwd(k):
        return rdma(sg_half(1, k), sg_half(1, k), zs.at[2, k], zr.at[2, k], partner)

    def g_load(k, fin):
        if fin:
            px(k, 1).wait_recv()
            py(k, 1).wait_recv()
            for cp in mid_sends(k):
                cp.wait_recv()
        else:
            px(k, 0).wait_recv()
            py(k, 0).wait_recv()
        for cp in ab_loads(k, fin):
            cp.start()

    def g_add(k, fin):
        for cp in ab_loads(k, fin):
            cp.wait()
        per = 3 if fin else 2

        def add(r, _):
            rows = pl.ds(pl.multiple_of(r * 48, 16), 48)
            for p in range(2):
                t = ab[per * p, rows, :].astype(F32)
                for e in range(1, per):
                    t = t + ab[per * p + e, rows, :].astype(F32)
                ob[p, rows, :] = t.astype(BF16)
            return 0
        lax.fori_loop(0, QR // 48, add, 0)
        for cp in ob_outs(k, fin):
            cp.start()

    def g_push(k, fin):
        for cp in ob_outs(k, fin):
            cp.wait()
        for cp in (z_sends(k) if fin else mid_sends(k)):
            cp.start()

    for cp in lw + lx:
        cp.start()
    g1_load(0).start()
    bar = pltpu.get_barrier_semaphore()
    for dev in (partner, xnbr, ynbr, znbr):
        pl.semaphore_signal(bar, inc=1, device_id=dev, device_id_type=MESH)
    pl.semaphore_wait(bar, 4)
    for cp in pw:
        cp.start()
    gw.start('x0', 'y1', 'x1', 'y0')

    def zero(r, _):
        acc[pl.ds(pl.multiple_of(r * 16, 16), 16), :] = jnp.zeros((16, T), F32)
        return 0
    lax.fori_loop(0, D // 16, zero, 0)

    for cp in lw + lx:
        cp.wait()
    for cp in pw:
        cp.wait_recv()

    def body(n, _):
        j = n // NI
        i = n % NI

        def at(k):
            return pl.when(n == k)

        @pl.when(n < 12)
        def _():
            g_stage1(n)

        @at(S2 - 1)
        def _():
            g1_send(0).wait_recv()
            for cp in g2_loads(0):
                cp.start()

        @pl.when((n > S2) & (n <= S2 + 12))
        def _():
            g_sends(n - S2 - 1)

        @pl.when((n >= S2) & (n < S2 + 12))
        def _():
            g_stage2(n - S2)

        @at(3)
        def _():
            gw.recv('x0')
            gw.start('zx0', 'yf')
            gw.recv('y1')
            gw.start('xf')

        @at(5)
        def _():
            gw.recv('x1')
            gw.start('zx1', 'zy1')
            gw.recv('y0')
            gw.start('zy0')
            for cp in lv + pv:
                cp.start()

        @at(8)
        def _():
            gw.recv('zx0', 'zx1')
            gw.start('dx')
            gw.recv('dx')

        @at(12)
        def _():
            g1_send(11).wait_send()
            gw.recv('xf', 'yf')
            gw.start('zd0', 'zd1')

        @at(15)
        def _():
            gw.recv('zy0', 'zy1')
            gw.start('dy')
            gvb.start('x0', 'y1')

        @at(16)
        def _():
            gw.recv('dy')

        @at(18)
        def _():
            gvb.start('x1', 'y0')

        @at(20)
        def _():
            gva.start('x0', 'y1', 'x1', 'y0')

        @at(22)
        def _():
            gw.recv('zd0', 'zd1')
            gw.start('dd')

        @at(24)
        def _():
            gw.recv('dd')
            gvb.recv('x0')
            gvb.start('yf')
            gvb.recv('y1')
            gvb.start('xf')

        @at(28)
        def _():
            gva.recv('x0')
            gva.start('yf', 'zx0')
            gva.recv('y1')
            gva.start('xf', 'zy1')
            gvb.recv('x1', 'y0')
            gvb.start('dx', 'dy')

        @at(30)
        def _():
            gva.recv('x1')
            gva.start('zx1')
            gva.recv('y0')
            gva.start('zy0')

        for e, (k, fin) in zip(G_AT, ((0, 0), (1, 0), (2, 0), (0, 1), (1, 1), (2, 1))):
            @at(e + 2)
            def _():
                g_push(k, fin)

            @at(e + 1)
            def _():
                g_add(k, fin)

            @at(e)
            def _():
                g_load(k, fin)

        q = jnp.where(j == 0, q_own, jnp.where(j == 1, q_x, jnp.where(j == 2, q_y, q_d)))
        base = pl.multiple_of(q * CH, CH)

        @pl.when(i == 0)
        def _():
            def tr(r, _):
                src = pl.ds(pl.multiple_of(base + r * 128, 128), 128)
                for a in range(2):
                    wt[:, pl.ds(pl.multiple_of(a * CH + r * 128, 128), 128)] = w_v[a, src, :].T
                return 0
            lax.fori_loop(0, CH // 128, tr, 0)

        cols = pl.ds(pl.multiple_of(i * TM, TM), TM)
        slot = n % 2

        def hcopies(slot):
            return [pltpu.make_async_copy(hbuf.at[slot, pl.ds(a * CH, CH), :],
                                          h3_hbm.at[a, pl.ds(base, CH), cols], hsem.at[slot, a]) for a in range(3)]

        @pl.when(n >= 2)
        def _():
            for cp in hcopies(slot):
                cp.wait()

        for r in range(CH // SUB):
            src = pl.ds(pl.multiple_of(base + r * SUB, 16), SUB)
            a = dotf(w_v[0, src, :], x_v[:, cols], NN)
            b = dotf(w_v[1, src, :], x_v[:, cols], NN)
            dh = dotf(w_v[2, src, :], dy_v[:, cols], NN)
            s = 1.0 / (1.0 + jnp.exp(-a))
            act = a * s
            hbuf[slot, r * SUB:(r + 1) * SUB, :] = (dh * b * s * (1.0 + a * (1.0 - s))).astype(BF16)
            hbuf[slot, CH + r * SUB:CH + (r + 1) * SUB, :] = (dh * act).astype(BF16)
            hbuf[slot, 2 * CH + r * SUB:2 * CH + (r + 1) * SUB, :] = (act * b).astype(BF16)
        for cp in hcopies(slot):
            cp.start()
        acc[:, cols] += dotf(wt[...], hbuf[slot, 0:2 * CH, :], NN)

        @pl.when(j == NC - 1)
        def _():
            x_v[:, cols] = acc[:, cols].astype(BF16)
            pltpu.make_async_copy(x_v.at[:, cols], dx_hbm.at[:, cols], xsem).start()
        return 0

    lax.fori_loop(0, NC * NI, body, 0)

    gva.recv('xf', 'yf')
    gva.start('zd0', 'zd1')
    gvb.recv('xf', 'yf')
    gvb.start('dd')
    for k in range(3):
        z_sends(k)[0].wait_recv()
        z_fwd(k).start()
    gva.recv('zx0', 'zx1', 'zy0', 'zy1')
    gva.start('dx', 'dy')
    for slot in range(2):
        for a in range(3):
            pltpu.make_async_copy(hbuf.at[slot, pl.ds(a * CH, CH), :],
                                  h3_hbm.at[a, pl.ds(0, CH), pl.ds(0, TM)], hsem.at[slot, a]).wait()
    pltpu.make_async_copy(x_v, dx_hbm, xsem).wait()
    gva.recv('zd0', 'zd1')
    gva.start('dd')
    for cp in lv:
        cp.wait()
    for cp in pv:
        cp.wait_recv()
    for k in range(3):
        z_sends(k)[1].wait_recv()
        z_fwd(k).wait_recv()
    gvb.recv('dx', 'dy', 'dd')
    gva.recv('dx', 'dy', 'dd')
    for cp in pw + pv:
        cp.wait_send()
    for g in (gw, gva, gvb):
        g.sent()
    for k in range(3):
        for m in range(2):
            px(k, m).wait_send()
            py(k, m).wait_send()
        for cp in mid_sends(k) + z_sends(k) + (z_fwd(k),):
            cp.wait_send()


def run_step(*args):
    hbm = pl.BlockSpec(memory_space=pltpu.MemorySpace.HBM)

    def out(*shape):
        return jax.ShapeDtypeStruct(shape, BF16)
    dma = pltpu.SemaphoreType.DMA
    return pl.pallas_call(
        step_kernel,
        out_shape=(out(3, F, T), out(D, T), out(3, F, D), out(2, 3, D, CH),
                   out(12, HR, CH), out(12, HR, CH), out(3, 2, QR, CH), out(3, 2, QR, CH),
                   out(3, QR, CH), out(3, QR, CH), out(3, QR, CH), out(3, QR, CH)),
        in_specs=[hbm] * 9,
        out_specs=(hbm,) * 12,
        scratch_shapes=[
            pltpu.VMEM((D, T), BF16), pltpu.VMEM((D, T), BF16), pltpu.VMEM((D, T), F32),
            pltpu.VMEM((3, F, D), BF16), pltpu.VMEM((D, 2 * CH), BF16),
            pltpu.VMEM((2, 3 * CH, TM), BF16),
            pltpu.VMEM((HR, CH), F32), pltpu.VMEM((HR, CH), BF16),
            pltpu.VMEM((HR, CH), F32), pltpu.VMEM((HR, CH), BF16), pltpu.VMEM((HR, CH), BF16),
            pltpu.VMEM((6, QR, CH), BF16), pltpu.VMEM((2, QR, CH), BF16),
            dma((8,)), dma((2, 3)), dma, dma((84,)), dma((84,)),
            dma, dma, dma((12,)), dma((3,)), dma((2, 3, 2)), dma((2, 3, 2)),
            dma((6,)), dma((2,)), dma((2, 3)), dma((2, 3)), dma((3, 3)), dma((3, 3)),
        ],
        compiler_params=pltpu.CompilerParams(collective_id=0, has_side_effects=True,
                                             vmem_limit_bytes=66_900_000),
        cost_estimate=pl.CostEstimate(flops=10 * T * D * F, bytes_accessed=200_000_000, transcendentals=T * F),
    )(*args)


def grad_kernel(x_ref, dy_ref, h3_ref, dx_ref, v_ref, sg_ref,
                dw_ref, dxo_ref, v1o_ref, v3o_ref, v2o_ref, dn_ref, gt):
    s = pl.program_id(0)
    c = lax.axis_index('fsdp') % 2
    for k, (lhs, vo) in enumerate(((x_ref, v1o_ref), (x_ref, v3o_ref), (dy_ref, v2o_ref))):
        @pl.when(s // 5 == k)
        def _():
            dxo_ref[...] = dx_ref[...]
            vo[...] = v_ref[0].T
            dw_ref[0, 0] = dotf(lhs[...], h3_ref[0], NT)

    @pl.when(s % 5 == 3)
    def _():
        for r in range(0, CH, 128):
            gt[r:r + 128, :] = (sg_ref[0, 0, :, r:r + 128].astype(F32) + sg_ref[1, 0, :, r:r + 128].astype(F32)).T
        dn_ref[0] = gt[pl.ds(pl.multiple_of(c * SH, 8), SH), :]


def run_grad(x, dy, h3, dx, v, sg):
    one = pl.Buffered(1)
    whole = pl.BlockSpec((D, T), lambda s: (0, 0), pipeline_mode=one)
    dxs = pl.BlockSpec((D // 15, T), lambda s: (s, 0))

    def vspec(k):
        return pl.BlockSpec((D, 512), lambda s: (0, jnp.clip(s - 5 * k, 0, 4)))
    return pl.pallas_call(
        grad_kernel,
        grid=(15,),
        out_shape=(jax.ShapeDtypeStruct((1, 3, D, F), F32), jax.ShapeDtypeStruct((D, T), BF16),
                   jax.ShapeDtypeStruct((D, F), BF16), jax.ShapeDtypeStruct((D, F), BF16),
                   jax.ShapeDtypeStruct((D, F), BF16), jax.ShapeDtypeStruct((3, SH, D), F32)),
        in_specs=[whole, whole, pl.BlockSpec((1, 512, T), lambda s: (s // 5, s % 5, 0)), dxs,
                  pl.BlockSpec((1, 512, D), lambda s: (s // 5, s % 5, 0)),
                  pl.BlockSpec((2, 1, D, CH), lambda s: (0, s // 5, 0, 0), pipeline_mode=one)],
        out_specs=(pl.BlockSpec((1, 1, D, 512), lambda s: (0, s // 5, 0, s % 5)), dxs, vspec(0), vspec(1), vspec(2),
                   pl.BlockSpec((1, SH, D), lambda s: (s // 5, 0, 0))),
        scratch_shapes=[pltpu.VMEM((CH, D), F32)],
        compiler_params=pltpu.CompilerParams(vmem_limit_bytes=64_000_000),
        cost_estimate=pl.CostEstimate(flops=6 * T * D * F, bytes_accessed=150_000_000, transcendentals=0),
    )(x, dy, h3, dx, v, sg)


def solution(mesh):
    def device_step(x, dy, w1, w3, w2, v1, v3, v2, g_next):
        xt, dyt = x.T, dy.T
        h3, dx, v, sg = run_step(xt, dyt, w1.T, w3.T, w2, v1.T, v3.T, v2, g_next[0])[:4]
        dw, dxo, v1o, v3o, v2o, dn = run_grad(xt, dyt, h3, dx, v, sg)
        return dxo.T, dn.transpose(0, 2, 1), dw, v1o, v3o, v2o.T

    row_spec = P(ALL_AXES, None)
    col_shard = P(None, FSDP_AXES)
    row_shard = P(FSDP_AXES, None)
    dev_spec = P(ALL_AXES, None, None, None)
    return jax.shard_map(
        device_step, mesh=mesh,
        in_specs=(row_spec, row_spec, col_shard, col_shard, row_shard, col_shard, col_shard, row_shard, dev_spec),
        out_specs=(row_spec, P(None, None, FSDP_AXES), dev_spec, P(), P(), P()),
        check_vma=False)
```

```python
import jax
import jax.numpy as jnp
from jax import lax
from jax.experimental import pallas as pl
from jax.experimental.pallas import tpu as pltpu
from jax.sharding import PartitionSpec as P

ALL_AXES = ('dp', 'col', 'fsdp')
FSDP_AXES = ('col', 'fsdp')
MESH = pl.DeviceIdType.MESH
BF16 = jnp.bfloat16
F32 = jnp.float32

D = 960
F = 2560
T = 4096
SH = F // 8
CH = F // 4
TM = 512
NI = T // TM
NC = 4
SUB = 320
HR = D // 2
QR = HR // 2
S2 = 2
G_AT = (9, 12, 15, 17, 19, 22)

NN = (((1,), (0,)), ((), ()))
NT = (((1,), (1,)), ((), ()))


def dotf(a, b, dims):
    return lax.dot_general(a, b, dims, preferred_element_type=F32)


def step_kernel(x_hbm, dy_hbm, w1_hbm, w3_hbm, w2_hbm, v1_hbm, v3_hbm, v2_hbm, g_hbm,
                h3_hbm, dw_hbm, dx_hbm, v_out, sg, r1, pp, rx, ry, rx2, ry2, sx, sy,
                x_v, dy_v, acc, w_v, wt, hbuf, h_v, dacc, gin1, gout1, gin2, rin, gout2, ab, ob,
                lsem, hsem, xsem, wsem, send, recv, g1l, g1s, g1r, g2l, gps, gpr, abl, obs, gms, gmr, zs, zr):
    z = lax.axis_index('dp')
    y = lax.axis_index('col')
    fs = lax.axis_index('fsdp')
    x = fs // 2
    c = fs % 2
    partner = {'fsdp': x * 2 + (1 - c)}
    xnbr = {'fsdp': (1 - x) * 2 + c}
    ynbr = {'col': 1 - y}
    znbr = {'dp': 1 - z}
    q_own = y * 2 + x
    q_x = y * 2 + (1 - x)
    q_y = (1 - y) * 2 + x
    q_d = (1 - y) * 2 + (1 - x)

    def rdma(src, dst, ssem, rsem, dev):
        return pltpu.make_async_remote_copy(src, dst, ssem, rsem, device_id=dev, device_id_type=MESH)

    def remote(src, dst, dev, k):
        return rdma(src, dst, send.at[k], recv.at[k], dev)

    class Gather:
        KINDS = ('x0', 'x1', 'y0', 'y1', 'xf', 'yf', 'dx', 'dy', 'dd', 'zx0', 'zx1', 'zy0', 'zy1', 'zd0', 'zd1')

        def __init__(self, base, srcs, dst, arrays, zsplit):
            self.base, self.srcs, self.dst, self.arrays, self.zsplit = base, srcs, dst, arrays, zsplit
            self.lo = z * 160 if zsplit else 0
            self.n = 160 if zsplit else 320

        def blk(self, a, q, lo, n):
            return self.dst.at[a, pl.ds(pl.multiple_of(q * CH + c * SH + lo, 16), n), :]

        def copy(self, kind, a):
            k = self.base + len(self.arrays) * self.KINDS.index(kind) + self.arrays.index(a)
            h = self.n // 2
            if kind in ('x0', 'x1', 'y0', 'y1'):
                lo = self.lo + h * int(kind[1])
                return remote(self.srcs[a].at[pl.ds(pl.multiple_of(lo, 16), h), :], self.blk(a, q_own, lo, h),
                              xnbr if kind[0] == 'x' else ynbr, k)
            if kind == 'yf':
                return remote(self.blk(a, q_x, self.lo, h), self.blk(a, q_x, self.lo, h), ynbr, k)
            if kind == 'xf':
                return remote(self.blk(a, q_y, self.lo + h, h), self.blk(a, q_y, self.lo + h, h), xnbr, k)
            q = {'x': q_x, 'y': q_y, 'd': q_d}[kind[1]]
            if kind[0] == 'z':
                b = self.blk(a, q, self.lo + h * int(kind[2]), h)
                return remote(b, b, znbr, k)
            return remote(self.blk(a, q, 0, SH), self.blk(a, q, 0, SH), partner, k)

        def start(self, *kinds):
            for kind in kinds:
                for a in self.arrays:
                    self.copy(kind, a).start()

        def recv(self, *kinds):
            for kind in kinds:
                for a in self.arrays:
                    self.copy(kind, a).wait_recv()

        def sent(self):
            for kind in self.KINDS[:15 if self.zsplit else 9]:
                for a in self.arrays:
                    self.copy(kind, a).wait_send()

    w_hbm = (w1_hbm, w3_hbm, w2_hbm)
    v_hbm = (v1_hbm, v3_hbm, v2_hbm)
    gw = Gather(0, w_hbm, w_v, (0, 1, 2), True)
    gva = Gather(45, v_hbm, v_out, (0,), True)
    gvb = Gather(60, v_hbm, v_out, (1, 2), False)

    def local(src, dst, k):
        return pltpu.make_async_copy(src, dst, lsem.at[k])

    pw = [remote(w_hbm[a], gw.blk(a, q_own, 0, SH), partner, 78 + a) for a in range(3)]
    pv = [remote(v_hbm[a], gva.blk(a, q_own, 0, SH), partner, 81 + a) for a in range(3)]
    lw = [local(w_hbm[a], gw.blk(a, q_own, 0, SH), a) for a in range(3)]
    lv = [local(v_hbm[a], gva.blk(a, q_own, 0, SH), 3 + a) for a in range(3)]
    lx = [local(x_hbm, x_v, 6), local(dy_hbm, dy_v, 7)]

    def cols_of(q):
        return pl.ds(pl.multiple_of(q * CH, 128), CH)

    def unit(u):
        k = jnp.where(u < 9, u // 3, u - 9)
        m = jnp.where(u < 9, u % 3, 3)
        q = jnp.where(m == 0, q_d, jnp.where(m == 1, q_x, jnp.where(m == 2, q_y, q_own)))
        return k, 4 * k + m, cols_of(q)

    def half(h):
        return pl.ds(pl.multiple_of(h * HR, 16), HR)

    def g1_load(u):
        k, _, cq = unit(u)
        return pltpu.make_async_copy(g_hbm.at[k, half(1 - c), cq], gin1, g1l)

    def g1_send(u):
        return rdma(gout1, r1.at[u], g1s, g1r.at[u], partner)

    def g2_loads(u):
        k, _, cq = unit(u)
        return (pltpu.make_async_copy(g_hbm.at[k, half(c), cq], gin2, g2l.at[0]),
                pltpu.make_async_copy(r1.at[u], rin, g2l.at[1]))

    def g2_out(u):
        _, km, _ = unit(u)
        return pltpu.make_async_copy(gout2, pp.at[km], g2l.at[2])

    def px(k, m):
        return rdma(pp.at[4 * k + m, pl.ds(0, QR), :], rx.at[k, m], gps.at[0, k, m], gpr.at[0, k, m], xnbr)

    def py(k, m):
        return rdma(pp.at[4 * k + 2 * m, pl.ds(QR, QR), :], ry.at[k, m], gps.at[1, k, m], gpr.at[1, k, m], ynbr)

    def g_stage1(u):
        @pl.when(u > 0)
        def _():
            g1_send(u - 1).wait_send()
        g1_load(u).wait()

        for r in range(0, HR, 48):
            gout1[r:r + 48, :] = gin1[r:r + 48, :].astype(BF16)
        g1_send(u).start()

        @pl.when(u < 11)
        def _():
            g1_load(u + 1).start()

    def g_sends(u):
        g2_out(u).wait()
        k = u // 3

        @pl.when((u < 9) & (u % 3 == 0))
        def _():
            px(k, 0).start()
            py(k, 0).start()

        @pl.when((u < 9) & (u % 3 == 1))
        def _():
            px(k, 1).start()

        @pl.when((u < 9) & (u % 3 == 2))
        def _():
            py(k, 1).start()

    def g_stage2(u):
        for cp in g2_loads(u):
            cp.wait()

        for r in range(0, HR, 48):
            gout2[r:r + 48, :] = (gin2[r:r + 48, :].astype(BF16).astype(F32) + rin[r:r + 48, :].astype(F32)).astype(BF16)
        g2_out(u).start()

        @pl.when(u < 11)
        def _():
            g1_send(u + 1).wait_recv()
            for cp in g2_loads(u + 1):
                cp.start()

    def mid_sends(k):
        return (rdma(sy.at[k], ry2.at[k], gms.at[0, k], gmr.at[0, k], ynbr),
                rdma(sx.at[k], rx2.at[k], gms.at[1, k], gmr.at[1, k], xnbr))

    def ab_loads(k, fin):
        lo, hi = pl.ds(0, QR), pl.ds(QR, QR)
        if fin:
            srcs = (pp.at[4 * k + 3, lo, :], rx.at[k, 1], ry2.at[k], pp.at[4 * k + 3, hi, :], ry.at[k, 1], rx2.at[k])
        else:
            srcs = (pp.at[4 * k + 2, lo, :], rx.at[k, 0], pp.at[4 * k + 1, hi, :], ry.at[k, 0])
        return [pltpu.make_async_copy(s, ab.at[n], abl.at[n]) for n, s in enumerate(srcs)]

    def sg_half(s, k):
        return sg.at[s, k, half(c), :]

    def ob_outs(k, fin):
        if fin:
            dst = [sg.at[0, k, pl.ds(pl.multiple_of(c * HR + p * QR, 16), QR), :] for p in range(2)]
        else:
            dst = [sy.at[k], sx.at[k]]
        return [pltpu.make_async_copy(ob.at[p], dst[p], obs.at[p]) for p in range(2)]

    def z_sends(k):
        return (rdma(sg_half(0, k), sg_half(1, k), zs.at[0, k], zr.at[0, k], znbr),
                rdma(sg_half(0, k), sg_half(0, k), zs.at[1, k], zr.at[1, k], partner))

    def z_fwd(k):
        return rdma(sg_half(1, k), sg_half(1, k), zs.at[2, k], zr.at[2, k], partner)

    def g_load(k, fin):
        if fin:
            px(k, 1).wait_recv()
            py(k, 1).wait_recv()
            for cp in mid_sends(k):
                cp.wait_recv()
        else:
            px(k, 0).wait_recv()
            py(k, 0).wait_recv()
        for cp in ab_loads(k, fin):
            cp.start()

    def g_add(k, fin):
        for cp in ab_loads(k, fin):
            cp.wait()
        per = 3 if fin else 2

        def add(r, _):
            rows = pl.ds(pl.multiple_of(r * 48, 16), 48)
            for p in range(2):
                t = ab[per * p, rows, :].astype(F32)
                for e in range(1, per):
                    t = t + ab[per * p + e, rows, :].astype(F32)
                ob[p, rows, :] = t.astype(BF16)
            return 0
        lax.fori_loop(0, QR // 48, add, 0)
        for cp in ob_outs(k, fin):
            cp.start()

    def g_push(k, fin):
        for cp in ob_outs(k, fin):
            cp.wait()
        for cp in (z_sends(k) if fin else mid_sends(k)):
            cp.start()

    for cp in lw + lx:
        cp.start()
    g1_load(0).start()
    bar = pltpu.get_barrier_semaphore()
    for dev in (partner, xnbr, ynbr, znbr):
        pl.semaphore_signal(bar, inc=1, device_id=dev, device_id_type=MESH)
    pl.semaphore_wait(bar, 4)
    for cp in pw:
        cp.start()
    gw.start('x0', 'y1', 'x1', 'y0')

    def zero(r, _):
        acc[pl.ds(pl.multiple_of(r * 16, 16), 16), :] = jnp.zeros((16, T), F32)
        return 0
    lax.fori_loop(0, D // 16, zero, 0)

    for cp in lw + lx:
        cp.wait()
    for cp in pw:
        cp.wait_recv()

    def body(n, _):
        j = n // NI
        i = n % NI

        def at(k):
            return pl.when(n == k)

        @pl.when(n < 12)
        def _():
            g_stage1(n)

        @at(S2 - 1)
        def _():
            g1_send(0).wait_recv()
            for cp in g2_loads(0):
                cp.start()

        @pl.when((n > S2) & (n <= S2 + 12))
        def _():
            g_sends(n - S2 - 1)

        @pl.when((n >= S2) & (n < S2 + 12))
        def _():
            g_stage2(n - S2)

        @at(2)
        def _():
            gw.recv('x0')
            gw.start('zx0')
            gw.start('yf')
            gw.recv('y1')
            gw.start('xf')

        @at(4)
        def _():
            gw.recv('x1')
            gw.start('zx1')
            gw.recv('y0')

        @at(5)
        def _():
            gw.start('zy1')
            gw.start('zy0')
            for cp in lv + pv:
                cp.start()

        @at(7)
        def _():
            gw.recv('zx0')
            gw.recv('zx1')
            gw.start('dx')

        @at(8)
        def _():
            gw.recv('dx')

        @at(10)
        def _():
            gw.recv('xf')
            gw.recv('yf')
            gw.start('zd0')
            gw.start('zd1')

        @at(12)
        def _():
            g1_send(11).wait_send()

        @at(13)
        def _():
            gvb.start('x0')
            gvb.start('y1')

        @at(14)
        def _():
            gw.recv('zy0')
            gw.recv('zy1')
            gw.start('dy')

        @at(16)
        def _():
            gw.recv('dy')
            gvb.start('x1')
            gvb.start('y0')

        @at(18)
        def _():
            gva.start('x0')
            gva.start('y1')
            gva.start('x1')
            gva.start('y0')

        @at(19)
        def _():
            gw.recv('zd0')
            gw.recv('zd1')
            gw.start('dd')

        @at(20)
        def _():
            gvb.recv('x0')
            gvb.start('yf')
            gvb.recv('y1')
            gvb.start('xf')

        @at(23)
        def _():
            gvb.recv('x1')
            gvb.recv('y0')
            gvb.start('dx')
            gvb.start('dy')

        @at(24)
        def _():
            gw.recv('dd')
            gva.recv('x0')
            gva.start('yf')
            gva.start('zx0')
            gva.recv('y1')
            gva.start('xf')
            gva.start('zy1')
            gva.recv('x1')
            gva.start('zx1')
            gva.recv('y0')
            gva.start('zy0')

        @at(26)
        def _():
            gvb.recv('xf')
            gvb.recv('yf')
            gvb.start('dd')

        @at(27)
        def _():
            gva.recv('xf')
            gva.recv('yf')
            gva.start('zd0')
            gva.start('zd1')
            z_sends(0)[0].wait_recv()
            z_fwd(0).start()

        @at(29)
        def _():
            gva.recv('zx0')
            gva.recv('zx1')
            gva.recv('zy0')
            gva.recv('zy1')
            gva.start('dx')
            gva.start('dy')
            z_sends(1)[0].wait_recv()
            z_fwd(1).start()

        @at(31)
        def _():
            gva.recv('zd0')
            gva.recv('zd1')
            gva.start('dd')

        for e, (k, fin) in zip(G_AT, ((0, 0), (1, 0), (2, 0), (0, 1), (1, 1), (2, 1))):
            @at(e + 2)
            def _():
                g_push(k, fin)

            @at(e + 1)
            def _():
                g_add(k, fin)

            @at(e)
            def _():
                g_load(k, fin)

        q = jnp.where(j == 0, q_own, jnp.where(j == 1, q_x, jnp.where(j == 2, q_y, q_d)))
        base = pl.multiple_of(q * CH, CH)

        @pl.when(i == 0)
        def _():
            def tr(r, _):
                src = pl.ds(pl.multiple_of(base + r * 128, 128), 128)
                for a in range(2):
                    wt[:, pl.ds(pl.multiple_of(a * CH + r * 128, 128), 128)] = w_v[a, src, :].T
                return 0
            lax.fori_loop(0, CH // 128, tr, 0)

        cols = pl.ds(pl.multiple_of(i * TM, TM), TM)
        slot = n % 2

        def hcopies(slot):
            return [pltpu.make_async_copy(hbuf.at[slot, pl.ds(a * CH, CH), :],
                                          h3_hbm.at[a, pl.ds(base, CH), cols], hsem.at[slot, a]) for a in range(2)]

        dw_copy = pltpu.make_async_copy(dacc, dw_hbm.at[:, pl.ds(base, CH)], wsem)

        @pl.when((i == 0) & (j > 0))
        def _():
            dw_copy.wait()

        @pl.when(n >= 2)
        def _():
            for cp in hcopies(slot):
                cp.wait()

        for r in range(CH // SUB):
            src = pl.ds(pl.multiple_of(base + r * SUB, 16), SUB)
            a = dotf(w_v[0, src, :], x_v[:, cols], NN)
            b = dotf(w_v[1, src, :], x_v[:, cols], NN)
            dh = dotf(w_v[2, src, :], dy_v[:, cols], NN)
            s = 1.0 / (1.0 + jnp.exp(-a))
            act = a * s
            hbuf[slot, r * SUB:(r + 1) * SUB, :] = (dh * b * s * (1.0 + a * (1.0 - s))).astype(BF16)
            hbuf[slot, CH + r * SUB:CH + (r + 1) * SUB, :] = (dh * act).astype(BF16)
            h_v[r * SUB:(r + 1) * SUB, :] = (act * b).astype(BF16)
        for cp in hcopies(slot):
            cp.start()
        acc[:, cols] += dotf(wt[...], hbuf[slot], NN)
        dacc[...] = jnp.where(i == 0, 0.0, dacc[...]) + dotf(dy_v[:, cols], h_v[...], NT)

        @pl.when(i == NI - 1)
        def _():
            dw_copy.start()

        @pl.when(j == NC - 1)
        def _():
            x_v[:, cols] = acc[:, cols].astype(BF16)
            pltpu.make_async_copy(x_v.at[:, cols], dx_hbm.at[:, cols], xsem).start()
        return 0

    lax.fori_loop(0, NC * NI, body, 0)

    z_sends(2)[0].wait_recv()
    z_fwd(2).start()
    pltpu.make_async_copy(dacc, dw_hbm.at[:, pl.ds(0, CH)], wsem).wait()
    for slot in range(2):
        for a in range(2):
            pltpu.make_async_copy(hbuf.at[slot, pl.ds(a * CH, CH), :],
                                  h3_hbm.at[a, pl.ds(0, CH), pl.ds(0, TM)], hsem.at[slot, a]).wait()
    pltpu.make_async_copy(x_v, dx_hbm, xsem).wait()
    for cp in lv:
        cp.wait()
    for cp in pv:
        cp.wait_recv()
    for k in range(3):
        z_sends(k)[1].wait_recv()
        z_fwd(k).wait_recv()
    gvb.recv('dx', 'dy', 'dd')
    gva.recv('dx', 'dy', 'dd')
    for cp in pw + pv:
        cp.wait_send()
    for g in (gw, gva, gvb):
        g.sent()
    for k in range(3):
        for m in range(2):
            px(k, m).wait_send()
            py(k, m).wait_send()
        for cp in mid_sends(k) + z_sends(k) + (z_fwd(k),):
            cp.wait_send()


def run_step(*args):
    hbm = pl.BlockSpec(memory_space=pltpu.MemorySpace.HBM)

    def out(*shape, dtype=BF16):
        return jax.ShapeDtypeStruct(shape, dtype)
    dma = pltpu.SemaphoreType.DMA
    return pl.pallas_call(
        step_kernel,
        out_shape=(out(2, F, T), out(D, F, dtype=F32), out(D, T), out(3, F, D), out(2, 3, D, CH),
                   out(12, HR, CH), out(12, HR, CH), out(3, 2, QR, CH), out(3, 2, QR, CH),
                   out(3, QR, CH), out(3, QR, CH), out(3, QR, CH), out(3, QR, CH)),
        in_specs=[hbm] * 9,
        out_specs=(hbm,) * 13,
        scratch_shapes=[
            pltpu.VMEM((D, T), BF16), pltpu.VMEM((D, T), BF16), pltpu.VMEM((D, T), F32),
            pltpu.VMEM((3, F, D), BF16), pltpu.VMEM((D, 2 * CH), BF16),
            pltpu.VMEM((2, 2 * CH, TM), BF16), pltpu.VMEM((CH, TM), BF16), pltpu.VMEM((D, CH), F32),
            pltpu.VMEM((HR, CH), F32), pltpu.VMEM((HR, CH), BF16),
            pltpu.VMEM((HR, CH), F32), pltpu.VMEM((HR, CH), BF16), pltpu.VMEM((HR, CH), BF16),
            pltpu.VMEM((6, QR, CH), BF16), pltpu.VMEM((2, QR, CH), BF16),
            dma((8,)), dma((2, 2)), dma, dma, dma((84,)), dma((84,)),
            dma, dma, dma((12,)), dma((3,)), dma((2, 3, 2)), dma((2, 3, 2)),
            dma((6,)), dma((2,)), dma((2, 3)), dma((2, 3)), dma((3, 3)), dma((3, 3)),
        ],
        compiler_params=pltpu.CompilerParams(collective_id=0, has_side_effects=True,
                                             vmem_limit_bytes=66_900_000),
        cost_estimate=pl.CostEstimate(flops=12 * T * D * F, bytes_accessed=200_000_000, transcendentals=T * F),
    )(*args)


def grad_kernel(x_ref, h3_ref, dwt_ref, dx_ref, v_ref, sg_ref,
                dw_hbm, dxo_ref, v1o_ref, v3o_ref, v2o_ref, dn_ref, ob, gt, osem, csem):
    s = pl.program_id(0)
    c = lax.axis_index('fsdp') % 2

    def out(s):
        return pltpu.make_async_copy(
            ob.at[s % 2], dw_hbm.at[0, s // 5, :, pl.ds(pl.multiple_of(s % 5 * 512, 512), 512)], osem.at[s % 2])

    def third(s):
        return pltpu.make_async_copy(dwt_ref, dw_hbm.at[0, 2, pl.ds(pl.multiple_of(s * 96, 8), 96), :], csem)

    third(s).start()

    @pl.when(s >= 2)
    def _():
        out(s - 2).wait()

    def main():
        dxo_ref[...] = dx_ref[...]
        for a, vo in enumerate((v1o_ref, v3o_ref, v2o_ref)):
            vo[...] = v_ref[a].T
        ob[s % 2] = dotf(x_ref[...], h3_ref[0], NT)

    @pl.when(s % 2 == 0)
    def _():
        rows = pl.ds(pl.multiple_of(s // 2 * 128, 128), 128)
        for k in range(3):
            gt[k, rows, :] = (sg_ref[0, k].astype(F32) + sg_ref[1, k].astype(F32)).T
        main()

    @pl.when(s % 2 == 1)
    def _():
        main()

    out(s).start()
    third(s).wait()

    @pl.when(s == 9)
    def _():
        dn_ref[...] = gt[:, pl.ds(pl.multiple_of(c * SH, 8), SH), :]
        out(8).wait()
        out(9).wait()


def run_grad(x, h3, dwt, dx, v, sg):
    one = pl.Buffered(1)
    dxs = pl.BlockSpec((D // 10, T), lambda s: (s, 0))
    vs = pl.BlockSpec((D, 256), lambda s: (0, s))
    return pl.pallas_call(
        grad_kernel,
        grid=(10,),
        out_shape=(jax.ShapeDtypeStruct((1, 3, D, F), F32), jax.ShapeDtypeStruct((D, T), BF16),
                   jax.ShapeDtypeStruct((D, F), BF16), jax.ShapeDtypeStruct((D, F), BF16),
                   jax.ShapeDtypeStruct((D, F), BF16), jax.ShapeDtypeStruct((3, SH, D), F32)),
        in_specs=[pl.BlockSpec((D, T), lambda s: (0, 0), pipeline_mode=one),
                  pl.BlockSpec((1, 512, T), lambda s: (s // 5, s % 5, 0)),
                  pl.BlockSpec((D // 10, F), lambda s: (s, 0)), dxs,
                  pl.BlockSpec((3, 256, D), lambda s: (0, s, 0)),
                  pl.BlockSpec((2, 3, D, 128), lambda s: (0, 0, 0, s // 2))],
        out_specs=(pl.BlockSpec(memory_space=pltpu.MemorySpace.HBM), dxs, vs, vs, vs,
                   pl.BlockSpec((3, SH, D), lambda s: (0, 0, 0), pipeline_mode=one)),
        scratch_shapes=[pltpu.VMEM((2, D, 512), F32), pltpu.VMEM((3, CH, D), F32),
                        pltpu.SemaphoreType.DMA((2,)), pltpu.SemaphoreType.DMA],
        compiler_params=pltpu.CompilerParams(vmem_limit_bytes=64_000_000),
        cost_estimate=pl.CostEstimate(flops=4 * T * D * F, bytes_accessed=150_000_000, transcendentals=0),
    )(x, h3, dwt, dx, v, sg)


def solution(mesh):
    def device_step(x, dy, w1, w3, w2, v1, v3, v2, g_next):
        xt, dyt = x.T, dy.T
        h3, dwt, dx, v, sg = run_step(xt, dyt, w1.T, w3.T, w2, v1.T, v3.T, v2, g_next[0])[:5]
        dw, dxo, v1o, v3o, v2o, dn = run_grad(xt, h3, dwt, dx, v, sg)
        return dxo.T, dn.transpose(0, 2, 1), dw, v1o, v3o, v2o.T

    row_spec = P(ALL_AXES, None)
    col_shard = P(None, FSDP_AXES)
    row_shard = P(FSDP_AXES, None)
    dev_spec = P(ALL_AXES, None, None, None)
    return jax.shard_map(
        device_step, mesh=mesh,
        in_specs=(row_spec, row_spec, col_shard, col_shard, row_shard, col_shard, col_shard, row_shard, dev_spec),
        out_specs=(row_spec, P(None, None, FSDP_AXES), dev_spec, P(), P(), P()),
        check_vma=False)
```

```python
import functools

import jax
import jax.numpy as jnp
from jax import lax
from jax.experimental import pallas as pl
from jax.experimental.pallas import tpu as pltpu
from jax.sharding import PartitionSpec as P

ALL_AXES = ('dp', 'col', 'fsdp')
FSDP_AXES = ('col', 'fsdp')
MESH = pl.DeviceIdType.MESH
BF16 = jnp.bfloat16
F32 = jnp.float32

D = 960
F = 2560
T = 4096
SH = F // 8
CH = F // 4
TM = 512
NI = T // TM
NC = 4
SUB = 320
HR = D // 2
QR = HR // 2
RB = D // 10
S2 = 2
G_AT = (9, 12, 15, 18, 21, 24)

NN = (((1,), (0,)), ((), ()))
NT = (((1,), (1,)), ((), ()))


def dotf(a, b, dims):
    return lax.dot_general(a, b, dims, preferred_element_type=F32)


def step_kernel(x_hbm, dy_hbm, w1_hbm, w3_hbm, w2_hbm, v1_hbm, v3_hbm, v2_hbm, g_hbm,
                h3_hbm, dw_hbm, dx_hbm, v_out, sg, r1, pp, rx, ry, rx2, ry2, sx, sy,
                x_v, dy_v, acc, w_v, wt, hbuf, h_v, dacc, gin1, gout1, gin2, rin, gout2, ab, ob,
                lsem, xl, hsem, xsem, wsem, send, recv, g1l, g1s, g1r, g2l, gps, gpr, abl, obs, gms, gmr, zs, zr):
    z = lax.axis_index('dp')
    y = lax.axis_index('col')
    fs = lax.axis_index('fsdp')
    x = fs // 2
    c = fs % 2
    partner = {'fsdp': x * 2 + (1 - c)}
    xnbr = {'fsdp': (1 - x) * 2 + c}
    ynbr = {'col': 1 - y}
    znbr = {'dp': 1 - z}
    q_own = y * 2 + x
    q_x = y * 2 + (1 - x)
    q_y = (1 - y) * 2 + x
    q_d = (1 - y) * 2 + (1 - x)

    def rdma(src, dst, ssem, rsem, dev):
        return pltpu.make_async_remote_copy(src, dst, ssem, rsem, device_id=dev, device_id_type=MESH)

    def remote(src, dst, dev, k):
        return rdma(src, dst, send.at[k], recv.at[k], dev)

    class Gather:
        KINDS = ('x0', 'x1', 'y0', 'y1', 'xf', 'yf', 'dx', 'dy', 'dd', 'zx0', 'zx1', 'zy0', 'zy1', 'zd0', 'zd1')

        def __init__(self, base, srcs, dst, arrays, zsplit):
            self.base, self.srcs, self.dst, self.arrays, self.zsplit = base, srcs, dst, arrays, zsplit
            self.lo = z * 160 if zsplit else 0
            self.n = 160 if zsplit else 320

        def blk(self, a, q, lo, n):
            return self.dst.at[a, pl.ds(pl.multiple_of(q * CH + c * SH + lo, 16), n), :]

        def copy(self, kind, a):
            k = self.base + len(self.arrays) * self.KINDS.index(kind) + self.arrays.index(a)
            h = self.n // 2
            if kind in ('x0', 'x1', 'y0', 'y1'):
                lo = self.lo + h * int(kind[1])
                return remote(self.srcs[a].at[pl.ds(pl.multiple_of(lo, 16), h), :], self.blk(a, q_own, lo, h),
                              xnbr if kind[0] == 'x' else ynbr, k)
            if kind == 'yf':
                return remote(self.blk(a, q_x, self.lo, h), self.blk(a, q_x, self.lo, h), ynbr, k)
            if kind == 'xf':
                return remote(self.blk(a, q_y, self.lo + h, h), self.blk(a, q_y, self.lo + h, h), xnbr, k)
            q = {'x': q_x, 'y': q_y, 'd': q_d}[kind[1]]
            if kind[0] == 'z':
                b = self.blk(a, q, self.lo + h * int(kind[2]), h)
                return remote(b, b, znbr, k)
            return remote(self.blk(a, q, 0, SH), self.blk(a, q, 0, SH), partner, k)

        def start(self, *kinds):
            for kind in kinds:
                for a in self.arrays:
                    self.copy(kind, a).start()

        def recv(self, *kinds):
            for kind in kinds:
                for a in self.arrays:
                    self.copy(kind, a).wait_recv()

        def sent(self):
            for kind in self.KINDS[:15 if self.zsplit else 9]:
                for a in self.arrays:
                    self.copy(kind, a).wait_send()

    w_hbm = (w1_hbm, w3_hbm, w2_hbm)
    v_hbm = (v1_hbm, v3_hbm, v2_hbm)
    gw = Gather(0, w_hbm, w_v, (0, 1, 2), True)
    gva = Gather(45, v_hbm, v_out, (0,), True)
    gvb = Gather(60, v_hbm, v_out, (1, 2), False)

    def local(src, dst, k):
        return pltpu.make_async_copy(src, dst, lsem.at[k])

    pw = [remote(w_hbm[a], gw.blk(a, q_own, 0, SH), partner, 78 + a) for a in range(3)]
    pv = [remote(v_hbm[a], gva.blk(a, q_own, 0, SH), partner, 81 + a) for a in range(3)]
    lw = [local(w_hbm[a], gw.blk(a, q_own, 0, SH), a) for a in range(3)]
    lv = [local(v_hbm[a], gva.blk(a, q_own, 0, SH), 3 + a) for a in range(3)]

    def lx(i):
        cols = pl.ds(pl.multiple_of(i * TM, TM), TM)
        return [pltpu.make_async_copy(src.at[:, cols], dst.at[:, cols], xl.at[k, i])
                for k, (src, dst) in enumerate(((x_hbm, x_v), (dy_hbm, dy_v)))]

    def cols_of(q):
        return pl.ds(pl.multiple_of(q * CH, 128), CH)

    def unit(u):
        k = jnp.where(u < 9, u // 3, u - 9)
        m = jnp.where(u < 9, u % 3, 3)
        q = jnp.where(m == 0, q_d, jnp.where(m == 1, q_x, jnp.where(m == 2, q_y, q_own)))
        return k, 4 * k + m, cols_of(q)

    def half(h):
        return pl.ds(pl.multiple_of(h * HR, 16), HR)

    def g1_load(u):
        k, _, cq = unit(u)
        return pltpu.make_async_copy(g_hbm.at[k, half(1 - c), cq], gin1, g1l)

    def g1_send(u):
        return rdma(gout1, r1.at[u], g1s, g1r.at[u], partner)

    def g2_loads(u):
        k, _, cq = unit(u)
        return (pltpu.make_async_copy(g_hbm.at[k, half(c), cq], gin2, g2l.at[0]),
                pltpu.make_async_copy(r1.at[u], rin, g2l.at[1]))

    def g2_out(u):
        _, km, _ = unit(u)
        return pltpu.make_async_copy(gout2, pp.at[km], g2l.at[2])

    def px(k, m):
        return rdma(pp.at[4 * k + m, pl.ds(0, QR), :], rx.at[k, m], gps.at[0, k, m], gpr.at[0, k, m], xnbr)

    def py(k, m):
        return rdma(pp.at[4 * k + 2 * m, pl.ds(QR, QR), :], ry.at[k, m], gps.at[1, k, m], gpr.at[1, k, m], ynbr)

    def g_stage1(u):
        g1_load(u).wait()

        for r in range(0, HR, 48):
            gout1[r:r + 48, :] = gin1[r:r + 48, :].astype(BF16)
        g1_send(u).start()

        @pl.when(u < 11)
        def _():
            g1_load(u + 1).start()

    def g_sends(u):
        g2_out(u).wait()
        k = u // 3

        @pl.when((u < 9) & (u % 3 == 0))
        def _():
            px(k, 0).start()
            py(k, 0).start()

        @pl.when((u < 9) & (u % 3 == 1))
        def _():
            px(k, 1).start()

        @pl.when((u < 9) & (u % 3 == 2))
        def _():
            py(k, 1).start()

    def g_stage2(u):
        for cp in g2_loads(u):
            cp.wait()

        for r in range(0, HR, 48):
            gout2[r:r + 48, :] = (gin2[r:r + 48, :].astype(BF16).astype(F32) + rin[r:r + 48, :].astype(F32)).astype(BF16)
        g2_out(u).start()

        @pl.when(u < 11)
        def _():
            g1_send(u + 1).wait_recv()
            for cp in g2_loads(u + 1):
                cp.start()

    def mid_sends(k):
        return (rdma(sy.at[k], ry2.at[k], gms.at[0, k], gmr.at[0, k], ynbr),
                rdma(sx.at[k], rx2.at[k], gms.at[1, k], gmr.at[1, k], xnbr))

    def ab_loads(k, fin):
        lo, hi = pl.ds(0, QR), pl.ds(QR, QR)
        if fin:
            srcs = (pp.at[4 * k + 3, lo, :], rx.at[k, 1], ry2.at[k], pp.at[4 * k + 3, hi, :], ry.at[k, 1], rx2.at[k])
        else:
            srcs = (pp.at[4 * k + 2, lo, :], rx.at[k, 0], pp.at[4 * k + 1, hi, :], ry.at[k, 0])
        return [pltpu.make_async_copy(s, ab.at[n], abl.at[n]) for n, s in enumerate(srcs)]

    def sg_half(s, k):
        return sg.at[s, k, half(c), :]

    def ob_outs(k, fin):
        if fin:
            dst = [sg.at[0, k, pl.ds(pl.multiple_of(c * HR + p * QR, 16), QR), :] for p in range(2)]
        else:
            dst = [sy.at[k], sx.at[k]]
        return [pltpu.make_async_copy(ob.at[p], dst[p], obs.at[p]) for p in range(2)]

    def z_sends(k):
        return (rdma(sg_half(0, k), sg_half(1, k), zs.at[0, k], zr.at[0, k], znbr),
                rdma(sg_half(0, k), sg_half(0, k), zs.at[1, k], zr.at[1, k], partner))

    def z_fwd(k):
        return rdma(sg_half(1, k), sg_half(1, k), zs.at[2, k], zr.at[2, k], partner)

    def g_load(k, fin):
        if fin:
            px(k, 1).wait_recv()
            py(k, 1).wait_recv()
            for cp in mid_sends(k):
                cp.wait_recv()
        else:
            px(k, 0).wait_recv()
            py(k, 0).wait_recv()
        for cp in ab_loads(k, fin):
            cp.start()

    def g_add(k, fin):
        for cp in ab_loads(k, fin):
            cp.wait()
        per = 3 if fin else 2

        def add(r, _):
            rows = pl.ds(pl.multiple_of(r * 48, 16), 48)
            for p in range(2):
                t = ab[per * p, rows, :].astype(F32)
                for e in range(1, per):
                    t = t + ab[per * p + e, rows, :].astype(F32)
                ob[p, rows, :] = t.astype(BF16)
            return 0
        lax.fori_loop(0, QR // 48, add, 0)
        for cp in ob_outs(k, fin):
            cp.start()

    def g_push(k, fin):
        for cp in ob_outs(k, fin):
            cp.wait()
        for cp in (z_sends(k) if fin else mid_sends(k)):
            cp.start()

    for cp in lw + lx(0):
        cp.start()
    g1_load(0).start()
    bar = pltpu.get_barrier_semaphore()
    for dev in (partner, xnbr, ynbr, znbr):
        pl.semaphore_signal(bar, inc=1, device_id=dev, device_id_type=MESH)
    pl.semaphore_wait(bar, 4)
    for cp in pw:
        cp.start()
    gw.start('x0', 'y1', 'x1', 'y0')
    for i in range(1, NI):
        for cp in lx(i):
            cp.start()
    for cp in lw:
        cp.wait()
    for cp in pw:
        cp.wait_recv()

    def body(n, _):
        j = n // NI
        i = n % NI

        @pl.when((n > 0) & (n <= 12))
        def _():
            g1_send(n - 1).wait_send()

        @pl.when(n <= S2 + 12)
        def _():
            @pl.when(n < 12)
            def _():
                g_stage1(n)

            @pl.when(n == S2 - 1)
            def _():
                g1_send(0).wait_recv()
                for cp in g2_loads(0):
                    cp.start()

            @pl.when(n > S2)
            def _():
                g_sends(n - S2 - 1)

            @pl.when((n >= S2) & (n < S2 + 12))
            def _():
                g_stage2(n - S2)

        steps = {}

        def at(k):
            def put(f):
                steps.setdefault(k, []).append(f)
            return put

        @at(2)
        def _():
            gw.recv('x0')
            gw.start('zx0', 'yf')
            gw.recv('y1')
            gw.start('xf')

        @at(4)
        def _():
            gw.recv('x1')
            gw.start('zx1')
            gw.recv('y0')

        @at(5)
        def _():
            gw.start('zy1', 'zy0')
            for cp in lv + pv:
                cp.start()

        @at(6)
        def _():
            gva.start('x0', 'y1', 'x1', 'y0')

        @at(7)
        def _():
            gw.recv('zx0', 'zx1')
            gw.start('dx')

        @at(8)
        def _():
            gw.recv('dx')

        @at(10)
        def _():
            gw.recv('xf', 'yf')
            gw.start('zd0', 'zd1')

        @at(11)
        def _():
            gva.recv('x0')
            gva.start('yf', 'zx0')
            gva.recv('y1')
            gva.start('xf', 'zy1')
            gva.recv('x1')
            gva.start('zx1')
            gva.recv('y0')
            gva.start('zy0')

        @at(14)
        def _():
            gw.recv('zy0', 'zy1')
            gw.start('dy')

        @at(16)
        def _():
            gw.recv('dy')
            gva.recv('xf', 'yf')
            gva.start('zd0', 'zd1')
            gvb.start('x0', 'y1')

        @at(19)
        def _():
            gw.recv('zd0', 'zd1')
            gw.start('dd')
            gvb.start('x1', 'y0')

        @at(20)
        def _():
            gva.recv('zx0', 'zx1', 'zy0', 'zy1')
            gva.start('dx', 'dy')
            gva.recv('zd0', 'zd1')
            gva.start('dd')

        @at(23)
        def _():
            gvb.recv('x0')
            gvb.start('yf')
            gvb.recv('y1')
            gvb.start('xf')

        @at(24)
        def _():
            gw.recv('dd')

        @at(25)
        def _():
            z_sends(0)[0].wait_recv()
            z_fwd(0).start()

        @at(27)
        def _():
            gvb.recv('x1', 'y0')
            gvb.start('dx', 'dy')

        @at(28)
        def _():
            z_sends(1)[0].wait_recv()
            z_fwd(1).start()

        @at(30)
        def _():
            gvb.recv('xf', 'yf')
            gvb.start('dd')

        @at(31)
        def _():
            z_sends(2)[0].wait_recv()
            z_fwd(2).start()

        for e, (k, fin) in zip(G_AT, ((0, 0), (1, 0), (2, 0), (0, 1), (1, 1), (2, 1))):
            at(e + 2)(functools.partial(g_push, k, fin))
            at(e + 1)(functools.partial(g_add, k, fin))
            at(e)(functools.partial(g_load, k, fin))

        for jj in range(NC):
            @pl.when(j == jj)
            def _():
                for ii in range(NI):
                    if jj * NI + ii in steps:
                        @pl.when(i == ii)
                        def _():
                            for f in steps[jj * NI + ii]:
                                f()

        q = jnp.where(j == 0, q_own, jnp.where(j == 1, q_x, jnp.where(j == 2, q_y, q_d)))
        base = pl.multiple_of(q * CH, CH)

        @pl.when(i == 0)
        def _():
            def tr(r, _):
                src = pl.ds(pl.multiple_of(base + r * 128, 128), 128)
                for a in range(2):
                    wt[:, pl.ds(pl.multiple_of(a * CH + r * 128, 128), 128)] = w_v[a, src, :].T
                return 0
            lax.fori_loop(0, CH // 128, tr, 0)

        cols = pl.ds(pl.multiple_of(i * TM, TM), TM)
        slot = n % 2

        def hcopies(slot):
            return [pltpu.make_async_copy(hbuf.at[slot, pl.ds(a * CH, CH), :],
                                          h3_hbm.at[a, pl.ds(base, CH), cols], hsem.at[slot, a]) for a in range(2)]

        @pl.when(j == 0)
        def _():
            for cp in lx(i):
                cp.wait()

        dw_copy = pltpu.make_async_copy(dacc, dw_hbm.at[:, pl.ds(base, CH)], wsem)

        @pl.when((i == 0) & (j > 0))
        def _():
            dw_copy.wait()

        @pl.when(n >= 2)
        def _():
            for cp in hcopies(slot):
                cp.wait()

        for r in range(CH // SUB):
            src = pl.ds(pl.multiple_of(base + r * SUB, 16), SUB)
            a = dotf(w_v[0, src, :], x_v[:, cols], NN)
            b = dotf(w_v[1, src, :], x_v[:, cols], NN)
            dh = dotf(w_v[2, src, :], dy_v[:, cols], NN)
            s = 1.0 / (1.0 + jnp.exp(-a))
            act = a * s
            hbuf[slot, r * SUB:(r + 1) * SUB, :] = (dh * b * s * (1.0 + a * (1.0 - s))).astype(BF16)
            hbuf[slot, CH + r * SUB:CH + (r + 1) * SUB, :] = (dh * act).astype(BF16)
            h_v[r * SUB:(r + 1) * SUB, :] = (act * b).astype(BF16)
        for cp in hcopies(slot):
            cp.start()
        acc[:, cols] = jnp.where(j == 0, 0.0, acc[:, cols]) + dotf(wt[...], hbuf[slot], NN)
        dacc[...] = jnp.where(i == 0, 0.0, dacc[...]) + dotf(dy_v[:, cols], h_v[...], NT)

        @pl.when(i == NI - 1)
        def _():
            dw_copy.start()

        @pl.when(j == NC - 1)
        def _():
            x_v[:, cols] = acc[:, cols].astype(BF16)
            pltpu.make_async_copy(x_v.at[:, cols], dx_hbm.at[:, cols], xsem).start()
        return 0

    lax.fori_loop(0, NC * NI, body, 0)

    pltpu.make_async_copy(dacc, dw_hbm.at[:, pl.ds(0, CH)], wsem).wait()
    for slot in range(2):
        for a in range(2):
            pltpu.make_async_copy(hbuf.at[slot, pl.ds(a * CH, CH), :],
                                  h3_hbm.at[a, pl.ds(0, CH), pl.ds(0, TM)], hsem.at[slot, a]).wait()
    pltpu.make_async_copy(x_v, dx_hbm, xsem).wait()
    for cp in lv:
        cp.wait()
    for cp in pv:
        cp.wait_recv()
    for k in range(3):
        z_sends(k)[1].wait_recv()
        z_fwd(k).wait_recv()
    gvb.recv('dx', 'dy', 'dd')
    gva.recv('dx', 'dy', 'dd')
    for cp in pw + pv:
        cp.wait_send()
    for g in (gw, gva, gvb):
        g.sent()
    for k in range(3):
        for m in range(2):
            px(k, m).wait_send()
            py(k, m).wait_send()
        for cp in mid_sends(k) + z_sends(k) + (z_fwd(k),):
            cp.wait_send()


def run_step(*args):
    hbm = pl.BlockSpec(memory_space=pltpu.MemorySpace.HBM)

    def out(*shape, dtype=BF16):
        return jax.ShapeDtypeStruct(shape, dtype)
    dma = pltpu.SemaphoreType.DMA
    return pl.pallas_call(
        step_kernel,
        out_shape=(out(2, F, T), out(D, F, dtype=F32), out(D, T), out(3, F, D), out(2, 3, D, CH),
                   out(12, HR, CH), out(12, HR, CH), out(3, 2, QR, CH), out(3, 2, QR, CH),
                   out(3, QR, CH), out(3, QR, CH), out(3, QR, CH), out(3, QR, CH)),
        in_specs=[hbm] * 9,
        out_specs=(hbm,) * 13,
        scratch_shapes=[
            pltpu.VMEM((D, T), BF16), pltpu.VMEM((D, T), BF16), pltpu.VMEM((D, T), F32),
            pltpu.VMEM((3, F, D), BF16), pltpu.VMEM((D, 2 * CH), BF16),
            pltpu.VMEM((2, 2 * CH, TM), BF16), pltpu.VMEM((CH, TM), BF16), pltpu.VMEM((D, CH), F32),
            pltpu.VMEM((HR, CH), F32), pltpu.VMEM((HR, CH), BF16),
            pltpu.VMEM((HR, CH), F32), pltpu.VMEM((HR, CH), BF16), pltpu.VMEM((HR, CH), BF16),
            pltpu.VMEM((6, QR, CH), BF16), pltpu.VMEM((2, QR, CH), BF16),
            dma((6,)), dma((2, NI)), dma((2, 2)), dma, dma, dma((84,)), dma((84,)),
            dma, dma, dma((12,)), dma((3,)), dma((2, 3, 2)), dma((2, 3, 2)),
            dma((6,)), dma((2,)), dma((2, 3)), dma((2, 3)), dma((3, 3)), dma((3, 3)),
        ],
        compiler_params=pltpu.CompilerParams(collective_id=0, has_side_effects=True,
                                             vmem_limit_bytes=66_900_000),
        cost_estimate=pl.CostEstimate(flops=12 * T * D * F, bytes_accessed=200_000_000, transcendentals=T * F),
    )(*args)


def grad_kernel(x_hbm, h3_ref, dwt_hbm, dx_hbm, v_ref, sg_ref,
                dw_hbm, dxo_hbm, v1o_ref, v3o_ref, v2o_ref, dn_ref,
                xs, ob, gt, tb, db, xsem, osem, isem, esem):
    s = pl.program_id(0)
    c = lax.axis_index('fsdp') % 2

    def out(s):
        return pltpu.make_async_copy(
            ob.at[s % 2], dw_hbm.at[0, s // 5, :, pl.ds(pl.multiple_of(s % 5 * 512, 512), 512)], osem.at[s % 2])

    def rows(s):
        return pl.ds(pl.multiple_of(s * RB, 16), RB)

    def ins(s):
        return (pltpu.make_async_copy(dwt_hbm.at[rows(s), :], tb.at[s % 2], isem.at[0, s % 2]),
                pltpu.make_async_copy(dx_hbm.at[rows(s), :], db.at[s % 2], isem.at[1, s % 2]))

    def outs(s):
        return (pltpu.make_async_copy(tb.at[s % 2], dw_hbm.at[0, 2, rows(s), :], esem.at[0, s % 2]),
                pltpu.make_async_copy(db.at[s % 2], dxo_hbm.at[rows(s), :], esem.at[1, s % 2]))

    def xq(k):
        return pltpu.make_async_copy(x_hbm.at[:, k * 1024:(k + 1) * 1024], xs.at[:, k * 1024:(k + 1) * 1024], xsem.at[k])

    def turn_v():
        for a, vo in enumerate((v1o_ref, v3o_ref, v2o_ref)):
            vo[...] = v_ref[a].T

    def turn_g():
        r = pl.ds(pl.multiple_of(s // 2 * 128, 128), 128)
        for k in range(3):
            gt[k, r, :] = (sg_ref[0, k].astype(F32) + sg_ref[1, k].astype(F32)).T

    @pl.when(s >= 2)
    def _():
        out(s - 2).wait()

    @pl.when(s == 0)
    def _():
        for k in range(4):
            xq(k).start()
        for cp in ins(0):
            cp.start()
        turn_g()
        turn_v()
        for k in range(4):
            xq(k).wait()
            kq = slice(k * 1024, (k + 1) * 1024)
            part = dotf(xs[:, kq], h3_ref[0, :, kq], NT)
            ob[0] = part if k == 0 else ob[0] + part

    @pl.when((s > 0) & (s % 2 == 0))
    def _():
        turn_g()
        turn_v()
        ob[0] = dotf(xs[...], h3_ref[0], NT)

    @pl.when(s % 2 == 1)
    def _():
        turn_v()
        ob[1] = dotf(xs[...], h3_ref[0], NT)

    out(s).start()
    for cp in ins(s):
        cp.wait()
    for cp in outs(s):
        cp.start()

    @pl.when(s > 0)
    def _():
        for cp in outs(s - 1):
            cp.wait()

    @pl.when(s < 9)
    def _():
        for cp in ins(s + 1):
            cp.start()

    @pl.when(s == 9)
    def _():
        dn_ref[...] = gt[:, pl.ds(pl.multiple_of(c * SH, 8), SH), :]
        out(8).wait()
        out(9).wait()
        for cp in outs(9):
            cp.wait()


def run_grad(x, h3, dwt, dx, v, sg):
    hbm = pl.BlockSpec(memory_space=pltpu.MemorySpace.HBM)
    vs = pl.BlockSpec((D, 256), lambda s: (0, s))
    dma = pltpu.SemaphoreType.DMA
    return pl.pallas_call(
        grad_kernel,
        grid=(10,),
        out_shape=(jax.ShapeDtypeStruct((1, 3, D, F), F32), jax.ShapeDtypeStruct((D, T), BF16),
                   jax.ShapeDtypeStruct((D, F), BF16), jax.ShapeDtypeStruct((D, F), BF16),
                   jax.ShapeDtypeStruct((D, F), BF16), jax.ShapeDtypeStruct((3, SH, D), F32)),
        in_specs=[hbm, pl.BlockSpec((1, 512, T), lambda s: (s // 5, s % 5, 0)), hbm, hbm,
                  pl.BlockSpec((3, 256, D), lambda s: (0, s, 0)),
                  pl.BlockSpec((2, 3, D, 128), lambda s: (0, 0, 0, s // 2))],
        out_specs=(hbm, hbm, vs, vs, vs,
                   pl.BlockSpec((3, SH, D), lambda s: (0, 0, 0), pipeline_mode=pl.Buffered(1))),
        scratch_shapes=[pltpu.VMEM((D, T), BF16), pltpu.VMEM((2, D, 512), F32), pltpu.VMEM((3, CH, D), F32),
                        pltpu.VMEM((2, RB, F), F32), pltpu.VMEM((2, RB, T), BF16),
                        dma((4,)), dma((2,)), dma((2, 2)), dma((2, 2))],
        compiler_params=pltpu.CompilerParams(vmem_limit_bytes=64_000_000),
        cost_estimate=pl.CostEstimate(flops=4 * T * D * F, bytes_accessed=150_000_000, transcendentals=0),
    )(x, h3, dwt, dx, v, sg)


def solution(mesh):
    def device_step(x, dy, w1, w3, w2, v1, v3, v2, g_next):
        xt, dyt = x.T, dy.T
        h3, dwt, dx, v, sg = run_step(xt, dyt, w1.T, w3.T, w2, v1.T, v3.T, v2, g_next[0])[:5]
        dw, dxo, v1o, v3o, v2o, dn = run_grad(xt, h3, dwt, dx, v, sg)
        return dxo.T, dn.transpose(0, 2, 1), dw, v1o, v3o, v2o.T

    row_spec = P(ALL_AXES, None)
    col_shard = P(None, FSDP_AXES)
    row_shard = P(FSDP_AXES, None)
    dev_spec = P(ALL_AXES, None, None, None)
    return jax.shard_map(
        device_step, mesh=mesh,
        in_specs=(row_spec, row_spec, col_shard, col_shard, row_shard, col_shard, col_shard, row_shard, dev_spec),
        out_specs=(row_spec, P(None, None, FSDP_AXES), dev_spec, P(), P(), P()),
        check_vma=False)
```

```python
import functools

import jax
import jax.numpy as jnp
from jax import lax
from jax.experimental import pallas as pl
from jax.experimental.pallas import tpu as pltpu
from jax.sharding import PartitionSpec as P

ALL_AXES = ('dp', 'col', 'fsdp')
FSDP_AXES = ('col', 'fsdp')
MESH = pl.DeviceIdType.MESH
BF16 = jnp.bfloat16
F32 = jnp.float32

D = 960
F = 2560
T = 4096
SH = F // 8
CH = F // 4
TM = 512
NI = T // TM
NC = 4
SUB = 320
HR = D // 2
QR = HR // 2
RB = D // 10
S2 = 2
G_AT = (9, 12, 15, 18, 21, 24)

NN = (((1,), (0,)), ((), ()))
NT = (((1,), (1,)), ((), ()))


def dotf(a, b, dims):
    return lax.dot_general(a, b, dims, preferred_element_type=F32)


def step_kernel(x_hbm, dy_hbm, w1_hbm, w3_hbm, w2_hbm, v1_hbm, v3_hbm, v2_hbm, g_hbm,
                h3_hbm, dw_hbm, dx_hbm, v_out, sg, r1, pp, rx, ry, rx2, ry2, sx, sy,
                x_v, dy_v, acc, w_v, wt, hbuf, h_v, dacc, gin2, rin, gout2, ab, ob,
                lsem, xl, hsem, xsem, wsem, send, recv, g1s, g1r, g2l, gps, gpr, abl, obs, gms, gmr, zs, zr):
    z = lax.axis_index('dp')
    y = lax.axis_index('col')
    fs = lax.axis_index('fsdp')
    x = fs // 2
    c = fs % 2
    partner = {'fsdp': x * 2 + (1 - c)}
    xnbr = {'fsdp': (1 - x) * 2 + c}
    ynbr = {'col': 1 - y}
    znbr = {'dp': 1 - z}
    q_own = y * 2 + x
    q_x = y * 2 + (1 - x)
    q_y = (1 - y) * 2 + x
    q_d = (1 - y) * 2 + (1 - x)

    def rdma(src, dst, ssem, rsem, dev):
        return pltpu.make_async_remote_copy(src, dst, ssem, rsem, device_id=dev, device_id_type=MESH)

    def remote(src, dst, dev, k):
        return rdma(src, dst, send.at[k], recv.at[k], dev)

    class Gather:
        KINDS = ('x0', 'x1', 'y0', 'y1', 'xf', 'yf', 'dx', 'dy', 'dd', 'zx0', 'zx1', 'zy0', 'zy1', 'zd0', 'zd1')

        def __init__(self, base, srcs, dst, arrays, zsplit):
            self.base, self.srcs, self.dst, self.arrays, self.zsplit = base, srcs, dst, arrays, zsplit
            self.lo = z * 160 if zsplit else 0
            self.n = 160 if zsplit else 320

        def blk(self, a, q, lo, n):
            return self.dst.at[a, pl.ds(pl.multiple_of(q * CH + c * SH + lo, 16), n), :]

        def copy(self, kind, a):
            k = self.base + len(self.arrays) * self.KINDS.index(kind) + self.arrays.index(a)
            h = self.n // 2
            if kind in ('x0', 'x1', 'y0', 'y1'):
                lo = self.lo + h * int(kind[1])
                return remote(self.srcs[a].at[pl.ds(pl.multiple_of(lo, 16), h), :], self.blk(a, q_own, lo, h),
                              xnbr if kind[0] == 'x' else ynbr, k)
            if kind == 'yf':
                return remote(self.blk(a, q_x, self.lo, h), self.blk(a, q_x, self.lo, h), ynbr, k)
            if kind == 'xf':
                return remote(self.blk(a, q_y, self.lo + h, h), self.blk(a, q_y, self.lo + h, h), xnbr, k)
            q = {'x': q_x, 'y': q_y, 'd': q_d}[kind[1]]
            if kind[0] == 'z':
                b = self.blk(a, q, self.lo + h * int(kind[2]), h)
                return remote(b, b, znbr, k)
            return remote(self.blk(a, q, 0, SH), self.blk(a, q, 0, SH), partner, k)

        def start(self, *kinds):
            for kind in kinds:
                for a in self.arrays:
                    self.copy(kind, a).start()

        def recv(self, *kinds):
            for kind in kinds:
                for a in self.arrays:
                    self.copy(kind, a).wait_recv()

        def sent(self):
            for kind in self.KINDS[:15 if self.zsplit else 9]:
                for a in self.arrays:
                    self.copy(kind, a).wait_send()

    w_hbm = (w1_hbm, w3_hbm, w2_hbm)
    v_hbm = (v1_hbm, v3_hbm, v2_hbm)
    gw = Gather(0, w_hbm, w_v, (0, 1, 2), True)
    gva = Gather(45, v_hbm, v_out, (0,), True)
    gvb = Gather(60, v_hbm, v_out, (1, 2), False)

    def local(src, dst, k):
        return pltpu.make_async_copy(src, dst, lsem.at[k])

    pw = [remote(w_hbm[a], gw.blk(a, q_own, 0, SH), partner, 78 + a) for a in range(3)]
    pv = [remote(v_hbm[a], gva.blk(a, q_own, 0, SH), partner, 81 + a) for a in range(3)]
    lw = [local(w_hbm[a], gw.blk(a, q_own, 0, SH), a) for a in range(3)]
    lv = [local(v_hbm[a], gva.blk(a, q_own, 0, SH), 3 + a) for a in range(3)]

    def lx(i):
        cols = pl.ds(pl.multiple_of(i * TM, TM), TM)
        return [pltpu.make_async_copy(src.at[:, cols], dst.at[:, cols], xl.at[k, i])
                for k, (src, dst) in enumerate(((x_hbm, x_v), (dy_hbm, dy_v)))]

    def cols_of(q):
        return pl.ds(pl.multiple_of(q * CH, 128), CH)

    def unit(u):
        k = jnp.where(u < 9, u // 3, u - 9)
        m = jnp.where(u < 9, u % 3, 3)
        q = jnp.where(m == 0, q_d, jnp.where(m == 1, q_x, jnp.where(m == 2, q_y, q_own)))
        return k, 4 * k + m, cols_of(q)

    def half(h):
        return pl.ds(pl.multiple_of(h * HR, 16), HR)

    def g1_send(u):
        k, _, cq = unit(u)
        return rdma(g_hbm.at[k, half(1 - c), cq], r1.at[u], g1s.at[u], g1r.at[u], partner)

    def g2_loads(u):
        k, _, cq = unit(u)
        return (pltpu.make_async_copy(g_hbm.at[k, half(c), cq], gin2, g2l.at[0]),
                pltpu.make_async_copy(r1.at[u], rin, g2l.at[1]))

    def g2_out(u):
        _, km, _ = unit(u)
        return pltpu.make_async_copy(gout2, pp.at[km], g2l.at[2])

    def px(k, m):
        return rdma(pp.at[4 * k + m, pl.ds(0, QR), :], rx.at[k, m], gps.at[0, k, m], gpr.at[0, k, m], xnbr)

    def py(k, m):
        return rdma(pp.at[4 * k + 2 * m, pl.ds(QR, QR), :], ry.at[k, m], gps.at[1, k, m], gpr.at[1, k, m], ynbr)

    def g_sends(u):
        g2_out(u).wait()
        k = u // 3

        @pl.when((u < 9) & (u % 3 == 0))
        def _():
            px(k, 0).start()
            py(k, 0).start()

        @pl.when((u < 9) & (u % 3 == 1))
        def _():
            px(k, 1).start()

        @pl.when((u < 9) & (u % 3 == 2))
        def _():
            py(k, 1).start()

    def g_stage2(u):
        for cp in g2_loads(u):
            cp.wait()

        for r in range(0, HR, 48):
            gout2[r:r + 48, :] = (gin2[r:r + 48, :].astype(BF16).astype(F32) + rin[r:r + 48, :].astype(BF16).astype(F32)).astype(BF16)
        g2_out(u).start()

        @pl.when(u < 11)
        def _():
            g1_send(u + 1).wait_recv()
            for cp in g2_loads(u + 1):
                cp.start()

    def mid_sends(k):
        return (rdma(sy.at[k], ry2.at[k], gms.at[0, k], gmr.at[0, k], ynbr),
                rdma(sx.at[k], rx2.at[k], gms.at[1, k], gmr.at[1, k], xnbr))

    def ab_loads(k, fin):
        lo, hi = pl.ds(0, QR), pl.ds(QR, QR)
        if fin:
            srcs = (pp.at[4 * k + 3, lo, :], rx.at[k, 1], ry2.at[k], pp.at[4 * k + 3, hi, :], ry.at[k, 1], rx2.at[k])
        else:
            srcs = (pp.at[4 * k + 2, lo, :], rx.at[k, 0], pp.at[4 * k + 1, hi, :], ry.at[k, 0])
        return [pltpu.make_async_copy(s, ab.at[n], abl.at[n]) for n, s in enumerate(srcs)]

    def sg_half(s, k):
        return sg.at[s, k, half(c), :]

    def ob_outs(k, fin):
        if fin:
            dst = [sg.at[0, k, pl.ds(pl.multiple_of(c * HR + p * QR, 16), QR), :] for p in range(2)]
        else:
            dst = [sy.at[k], sx.at[k]]
        return [pltpu.make_async_copy(ob.at[p], dst[p], obs.at[p]) for p in range(2)]

    def z_sends(k):
        return (rdma(sg_half(0, k), sg_half(1, k), zs.at[0, k], zr.at[0, k], znbr),
                rdma(sg_half(0, k), sg_half(0, k), zs.at[1, k], zr.at[1, k], partner))

    def z_fwd(k):
        return rdma(sg_half(1, k), sg_half(1, k), zs.at[2, k], zr.at[2, k], partner)

    def g_load(k, fin):
        if fin:
            px(k, 1).wait_recv()
            py(k, 1).wait_recv()
            for cp in mid_sends(k):
                cp.wait_recv()
        else:
            px(k, 0).wait_recv()
            py(k, 0).wait_recv()
        for cp in ab_loads(k, fin):
            cp.start()

    def g_add(k, fin):
        for cp in ab_loads(k, fin):
            cp.wait()
        per = 3 if fin else 2

        def add(r, _):
            rows = pl.ds(pl.multiple_of(r * 48, 16), 48)
            for p in range(2):
                t = ab[per * p, rows, :].astype(F32)
                for e in range(1, per):
                    t = t + ab[per * p + e, rows, :].astype(F32)
                ob[p, rows, :] = t.astype(BF16)
            return 0
        lax.fori_loop(0, QR // 48, add, 0)
        for cp in ob_outs(k, fin):
            cp.start()

    def g_push(k, fin):
        for cp in ob_outs(k, fin):
            cp.wait()
        for cp in (z_sends(k) if fin else mid_sends(k)):
            cp.start()

    for cp in lw + lx(0):
        cp.start()
    bar = pltpu.get_barrier_semaphore()
    for dev in (partner, xnbr, ynbr, znbr):
        pl.semaphore_signal(bar, inc=1, device_id=dev, device_id_type=MESH)
    pl.semaphore_wait(bar, 4)
    for cp in pw:
        cp.start()
    gw.start('x0', 'y1', 'x1', 'y0')
    for i in range(1, NI):
        for cp in lx(i):
            cp.start()
    for cp in lw:
        cp.wait()
    for cp in pw:
        cp.wait_recv()

    def body(n, _):
        j = n // NI
        i = n % NI

        @pl.when(n <= S2 + 12)
        def _():
            @pl.when(n == 0)
            def _():
                for u in range(12):
                    g1_send(u).start()

            @pl.when(n == S2 - 1)
            def _():
                g1_send(0).wait_recv()
                for cp in g2_loads(0):
                    cp.start()

            @pl.when(n > S2)
            def _():
                g_sends(n - S2 - 1)

            @pl.when((n >= S2) & (n < S2 + 12))
            def _():
                g_stage2(n - S2)

        steps = {}

        def at(k):
            def put(f):
                steps.setdefault(k, []).append(f)
            return put

        @at(2)
        def _():
            gw.recv('x0')
            gw.start('zx0', 'yf')
            gw.recv('y1')
            gw.start('xf')

        @at(4)
        def _():
            gw.recv('x1')
            gw.start('zx1')
            gw.recv('y0')

        @at(5)
        def _():
            gw.start('zy1', 'zy0')
            for cp in lv + pv:
                cp.start()

        @at(6)
        def _():
            gva.start('x0', 'y1', 'x1', 'y0')

        @at(7)
        def _():
            gw.recv('zx0', 'zx1')
            gw.start('dx')

        @at(8)
        def _():
            gw.recv('dx')

        @at(10)
        def _():
            gw.recv('xf', 'yf')
            gw.start('zd0', 'zd1')

        @at(11)
        def _():
            gva.recv('x0')
            gva.start('yf', 'zx0')
            gva.recv('y1')
            gva.start('xf', 'zy1')
            gva.recv('x1')
            gva.start('zx1')
            gva.recv('y0')
            gva.start('zy0')

        @at(14)
        def _():
            gw.recv('zy0', 'zy1')
            gw.start('dy')

        @at(16)
        def _():
            gw.recv('dy')
            gva.recv('xf', 'yf')
            gva.start('zd0', 'zd1')
            gvb.start('x0', 'y1')

        @at(19)
        def _():
            gw.recv('zd0', 'zd1')
            gw.start('dd')
            gvb.start('x1', 'y0')

        @at(20)
        def _():
            gva.recv('zx0', 'zx1', 'zy0', 'zy1')
            gva.start('dx', 'dy')
            gva.recv('zd0', 'zd1')
            gva.start('dd')

        @at(23)
        def _():
            gvb.recv('x0')
            gvb.start('yf')
            gvb.recv('y1')
            gvb.start('xf')

        @at(24)
        def _():
            gw.recv('dd')

        @at(25)
        def _():
            z_sends(0)[0].wait_recv()
            z_fwd(0).start()

        @at(27)
        def _():
            gvb.recv('x1', 'y0')
            gvb.start('dx', 'dy')

        @at(28)
        def _():
            z_sends(1)[0].wait_recv()
            z_fwd(1).start()

        @at(30)
        def _():
            gvb.recv('xf', 'yf')
            gvb.start('dd')

        @at(31)
        def _():
            z_sends(2)[0].wait_recv()
            z_fwd(2).start()

        for e, (k, fin) in zip(G_AT, ((0, 0), (1, 0), (2, 0), (0, 1), (1, 1), (2, 1))):
            at(e + 2)(functools.partial(g_push, k, fin))
            at(e + 1)(functools.partial(g_add, k, fin))
            at(e)(functools.partial(g_load, k, fin))

        for jj in range(NC):
            @pl.when(j == jj)
            def _():
                for ii in range(NI):
                    if jj * NI + ii in steps:
                        @pl.when(i == ii)
                        def _():
                            for f in steps[jj * NI + ii]:
                                f()

        q = jnp.where(j == 0, q_own, jnp.where(j == 1, q_x, jnp.where(j == 2, q_y, q_d)))
        base = pl.multiple_of(q * CH, CH)

        @pl.when(i == 0)
        def _():
            def tr(r, _):
                src = pl.ds(pl.multiple_of(base + r * 128, 128), 128)
                for a in range(2):
                    wt[:, pl.ds(pl.multiple_of(a * CH + r * 128, 128), 128)] = w_v[a, src, :].T
                return 0
            lax.fori_loop(0, CH // 128, tr, 0)

        cols = pl.ds(pl.multiple_of(i * TM, TM), TM)
        slot = n % 2

        def hcopies(slot):
            return [pltpu.make_async_copy(hbuf.at[slot, pl.ds(a * CH, CH), :],
                                          h3_hbm.at[a, pl.ds(base, CH), cols], hsem.at[slot, a]) for a in range(2)]

        @pl.when(j == 0)
        def _():
            for cp in lx(i):
                cp.wait()

        dw_copy = pltpu.make_async_copy(dacc, dw_hbm.at[:, pl.ds(base, CH)], wsem)

        @pl.when((i == 0) & (j > 0))
        def _():
            dw_copy.wait()

        @pl.when(n >= 2)
        def _():
            for cp in hcopies(slot):
                cp.wait()

        for r in range(CH // SUB):
            src = pl.ds(pl.multiple_of(base + r * SUB, 16), SUB)
            a = dotf(w_v[0, src, :], x_v[:, cols], NN)
            b = dotf(w_v[1, src, :], x_v[:, cols], NN)
            dh = dotf(w_v[2, src, :], dy_v[:, cols], NN)
            s = 1.0 / (1.0 + jnp.exp(-a))
            act = a * s
            hbuf[slot, r * SUB:(r + 1) * SUB, :] = (dh * b * s * (1.0 + a * (1.0 - s))).astype(BF16)
            hbuf[slot, CH + r * SUB:CH + (r + 1) * SUB, :] = (dh * act).astype(BF16)
            h_v[r * SUB:(r + 1) * SUB, :] = (act * b).astype(BF16)
        for cp in hcopies(slot):
            cp.start()
        acc[:, cols] = jnp.where(j == 0, 0.0, acc[:, cols]) + dotf(wt[...], hbuf[slot], NN)
        dacc[...] = jnp.where(i == 0, 0.0, dacc[...]) + dotf(dy_v[:, cols], h_v[...], NT)

        @pl.when(i == NI - 1)
        def _():
            dw_copy.start()

        @pl.when(j == NC - 1)
        def _():
            x_v[:, cols] = acc[:, cols].astype(BF16)
            pltpu.make_async_copy(x_v.at[:, cols], dx_hbm.at[:, cols], xsem).start()
        return 0

    lax.fori_loop(0, NC * NI, body, 0)

    pltpu.make_async_copy(dacc, dw_hbm.at[:, pl.ds(0, CH)], wsem).wait()
    for slot in range(2):
        for a in range(2):
            pltpu.make_async_copy(hbuf.at[slot, pl.ds(a * CH, CH), :],
                                  h3_hbm.at[a, pl.ds(0, CH), pl.ds(0, TM)], hsem.at[slot, a]).wait()
    pltpu.make_async_copy(x_v, dx_hbm, xsem).wait()
    for cp in lv:
        cp.wait()
    for cp in pv:
        cp.wait_recv()
    for k in range(3):
        z_sends(k)[1].wait_recv()
        z_fwd(k).wait_recv()
    gvb.recv('dx', 'dy', 'dd')
    gva.recv('dx', 'dy', 'dd')
    for cp in pw + pv + [g1_send(u) for u in range(12)]:
        cp.wait_send()
    for g in (gw, gva, gvb):
        g.sent()
    for k in range(3):
        for m in range(2):
            px(k, m).wait_send()
            py(k, m).wait_send()
        for cp in mid_sends(k) + z_sends(k) + (z_fwd(k),):
            cp.wait_send()


def run_step(*args):
    hbm = pl.BlockSpec(memory_space=pltpu.MemorySpace.HBM)

    def out(*shape, dtype=BF16):
        return jax.ShapeDtypeStruct(shape, dtype)
    dma = pltpu.SemaphoreType.DMA
    return pl.pallas_call(
        step_kernel,
        out_shape=(out(2, F, T), out(D, F, dtype=F32), out(D, T), out(3, F, D), out(2, 3, D, CH),
                   out(12, HR, CH, dtype=F32), out(12, HR, CH), out(3, 2, QR, CH), out(3, 2, QR, CH),
                   out(3, QR, CH), out(3, QR, CH), out(3, QR, CH), out(3, QR, CH)),
        in_specs=[hbm] * 9,
        out_specs=(hbm,) * 13,
        scratch_shapes=[
            pltpu.VMEM((D, T), BF16), pltpu.VMEM((D, T), BF16), pltpu.VMEM((D, T), F32),
            pltpu.VMEM((3, F, D), BF16), pltpu.VMEM((D, 2 * CH), BF16),
            pltpu.VMEM((2, 2 * CH, TM), BF16), pltpu.VMEM((CH, TM), BF16), pltpu.VMEM((D, CH), F32),
            pltpu.VMEM((HR, CH), F32), pltpu.VMEM((HR, CH), F32), pltpu.VMEM((HR, CH), BF16),
            pltpu.VMEM((6, QR, CH), BF16), pltpu.VMEM((2, QR, CH), BF16),
            dma((6,)), dma((2, NI)), dma((2, 2)), dma, dma, dma((84,)), dma((84,)),
            dma((12,)), dma((12,)), dma((3,)), dma((2, 3, 2)), dma((2, 3, 2)),
            dma((6,)), dma((2,)), dma((2, 3)), dma((2, 3)), dma((3, 3)), dma((3, 3)),
        ],
        compiler_params=pltpu.CompilerParams(collective_id=0, has_side_effects=True,
                                             vmem_limit_bytes=66_900_000),
        cost_estimate=pl.CostEstimate(flops=12 * T * D * F, bytes_accessed=200_000_000, transcendentals=T * F),
    )(*args)


def grad_kernel(x_hbm, h3_ref, dwt_hbm, dx_hbm, v_ref, sg_ref,
                dw_hbm, dxo_hbm, v1o_ref, v3o_ref, v2o_ref, dn_ref,
                xs, ob, gt, tb, db, xsem, osem, isem, esem):
    s = pl.program_id(0)
    c = lax.axis_index('fsdp') % 2

    def out(s):
        return pltpu.make_async_copy(
            ob.at[s % 2], dw_hbm.at[0, s // 5, :, pl.ds(pl.multiple_of(s % 5 * 512, 512), 512)], osem.at[s % 2])

    def rows(s):
        return pl.ds(pl.multiple_of(s * RB, 16), RB)

    def ins(s):
        return (pltpu.make_async_copy(dwt_hbm.at[rows(s), :], tb.at[s % 2], isem.at[0, s % 2]),
                pltpu.make_async_copy(dx_hbm.at[rows(s), :], db.at[s % 2], isem.at[1, s % 2]))

    def outs(s):
        return (pltpu.make_async_copy(tb.at[s % 2], dw_hbm.at[0, 2, rows(s), :], esem.at[0, s % 2]),
                pltpu.make_async_copy(db.at[s % 2], dxo_hbm.at[rows(s), :], esem.at[1, s % 2]))

    def xq(k):
        return pltpu.make_async_copy(x_hbm.at[:, k * 1024:(k + 1) * 1024], xs.at[:, k * 1024:(k + 1) * 1024], xsem.at[k])

    def turn_v():
        for a, vo in enumerate((v1o_ref, v3o_ref, v2o_ref)):
            vo[...] = v_ref[a].T

    def turn_g():
        r = pl.ds(pl.multiple_of(s // 2 * 128, 128), 128)
        for k in range(3):
            gt[k, r, :] = (sg_ref[0, k].astype(F32) + sg_ref[1, k].astype(F32)).T

    @pl.when(s >= 2)
    def _():
        out(s - 2).wait()

    @pl.when(s == 0)
    def _():
        for k in range(4):
            xq(k).start()
        for cp in ins(0):
            cp.start()
        turn_g()
        turn_v()
        for k in range(4):
            xq(k).wait()
            kq = slice(k * 1024, (k + 1) * 1024)
            part = dotf(xs[:, kq], h3_ref[0, :, kq], NT)
            ob[0] = part if k == 0 else ob[0] + part

    @pl.when((s > 0) & (s % 2 == 0))
    def _():
        turn_g()
        turn_v()
        ob[0] = dotf(xs[...], h3_ref[0], NT)

    @pl.when(s % 2 == 1)
    def _():
        turn_v()
        ob[1] = dotf(xs[...], h3_ref[0], NT)

    out(s).start()
    for cp in ins(s):
        cp.wait()
    for cp in outs(s):
        cp.start()

    @pl.when(s > 0)
    def _():
        for cp in outs(s - 1):
            cp.wait()

    @pl.when(s < 9)
    def _():
        for cp in ins(s + 1):
            cp.start()

    @pl.when(s == 9)
    def _():
        dn_ref[...] = gt[:, pl.ds(pl.multiple_of(c * SH, 8), SH), :]
        out(8).wait()
        out(9).wait()
        for cp in outs(9):
            cp.wait()


def run_grad(x, h3, dwt, dx, v, sg):
    hbm = pl.BlockSpec(memory_space=pltpu.MemorySpace.HBM)
    vs = pl.BlockSpec((D, 256), lambda s: (0, s))
    dma = pltpu.SemaphoreType.DMA
    return pl.pallas_call(
        grad_kernel,
        grid=(10,),
        out_shape=(jax.ShapeDtypeStruct((1, 3, D, F), F32), jax.ShapeDtypeStruct((D, T), BF16),
                   jax.ShapeDtypeStruct((D, F), BF16), jax.ShapeDtypeStruct((D, F), BF16),
                   jax.ShapeDtypeStruct((D, F), BF16), jax.ShapeDtypeStruct((3, SH, D), F32)),
        in_specs=[hbm, pl.BlockSpec((1, 512, T), lambda s: (s // 5, s % 5, 0)), hbm, hbm,
                  pl.BlockSpec((3, 256, D), lambda s: (0, s, 0)),
                  pl.BlockSpec((2, 3, D, 128), lambda s: (0, 0, 0, s // 2))],
        out_specs=(hbm, hbm, vs, vs, vs,
                   pl.BlockSpec((3, SH, D), lambda s: (0, 0, 0), pipeline_mode=pl.Buffered(1))),
        scratch_shapes=[pltpu.VMEM((D, T), BF16), pltpu.VMEM((2, D, 512), F32), pltpu.VMEM((3, CH, D), F32),
                        pltpu.VMEM((2, RB, F), F32), pltpu.VMEM((2, RB, T), BF16),
                        dma((4,)), dma((2,)), dma((2, 2)), dma((2, 2))],
        compiler_params=pltpu.CompilerParams(vmem_limit_bytes=64_000_000),
        cost_estimate=pl.CostEstimate(flops=4 * T * D * F, bytes_accessed=150_000_000, transcendentals=0),
    )(x, h3, dwt, dx, v, sg)


def solution(mesh):
    def device_step(x, dy, w1, w3, w2, v1, v3, v2, g_next):
        xt, dyt = x.T, dy.T
        h3, dwt, dx, v, sg = run_step(xt, dyt, w1.T, w3.T, w2, v1.T, v3.T, v2, g_next[0])[:5]
        dw, dxo, v1o, v3o, v2o, dn = run_grad(xt, h3, dwt, dx, v, sg)
        return dxo.T, dn.transpose(0, 2, 1), dw, v1o, v3o, v2o.T

    row_spec = P(ALL_AXES, None)
    col_shard = P(None, FSDP_AXES)
    row_shard = P(FSDP_AXES, None)
    dev_spec = P(ALL_AXES, None, None, None)
    return jax.shard_map(
        device_step, mesh=mesh,
        in_specs=(row_spec, row_spec, col_shard, col_shard, row_shard, col_shard, col_shard, row_shard, dev_spec),
        out_specs=(row_spec, P(None, None, FSDP_AXES), dev_spec, P(), P(), P()),
        check_vma=False)
```

```python
import functools

import jax
import jax.numpy as jnp
from jax import lax
from jax.experimental import pallas as pl
from jax.experimental.pallas import tpu as pltpu
from jax.sharding import PartitionSpec as P

ALL_AXES = ('dp', 'col', 'fsdp')
FSDP_AXES = ('col', 'fsdp')
MESH = pl.DeviceIdType.MESH
BF16 = jnp.bfloat16
F32 = jnp.float32

D = 960
F = 2560
T = 4096
SH = F // 8
CH = F // 4
TM = 512
NI = T // TM
NC = 4
SUB = 320
HR = D // 2
QR = HR // 2
RB = D // 10
S2 = 2
G_AT = (10, 11, 15, 18, 21, 24)

NN = (((1,), (0,)), ((), ()))
NT = (((1,), (1,)), ((), ()))


def dotf(a, b, dims):
    return lax.dot_general(a, b, dims, preferred_element_type=F32)


def step_kernel(x_hbm, dy_hbm, w1_hbm, w3_hbm, w2_hbm, v1_hbm, v3_hbm, v2_hbm, g_hbm,
                h3_hbm, dw_hbm, dx_hbm, v_out, sg, r1, pp, rx, ry, rx2, ry2, sx, sy,
                x_v, dy_v, acc, w_v, wt, hbuf, h_v, dacc, gin2, rin, gout2, ab, ob,
                lsem, xl, hsem, xsem, wsem, send, recv, g1s, g1r, g2l, gps, gpr, abl, obs, gms, gmr, zs, zr):
    z = lax.axis_index('dp')
    y = lax.axis_index('col')
    fs = lax.axis_index('fsdp')
    x = fs // 2
    c = fs % 2
    partner = {'fsdp': x * 2 + (1 - c)}
    xnbr = {'fsdp': (1 - x) * 2 + c}
    ynbr = {'col': 1 - y}
    znbr = {'dp': 1 - z}
    q_own = y * 2 + x
    q_x = y * 2 + (1 - x)
    q_y = (1 - y) * 2 + x
    q_d = (1 - y) * 2 + (1 - x)

    def rdma(src, dst, ssem, rsem, dev):
        return pltpu.make_async_remote_copy(src, dst, ssem, rsem, device_id=dev, device_id_type=MESH)

    def remote(src, dst, dev, k):
        return rdma(src, dst, send.at[k], recv.at[k], dev)

    class Gather:
        KINDS = ('x0', 'x1', 'y0', 'y1', 'xf', 'yf', 'dx', 'dy', 'dd', 'zx0', 'zx1', 'zy0', 'zy1', 'zd0', 'zd1')

        def __init__(self, base, srcs, dst, arrays, zsplit):
            self.base, self.srcs, self.dst, self.arrays, self.zsplit = base, srcs, dst, arrays, zsplit
            self.lo = z * 160 if zsplit else 0
            self.n = 160 if zsplit else 320

        def blk(self, a, q, lo, n):
            return self.dst.at[a, pl.ds(pl.multiple_of(q * CH + c * SH + lo, 16), n), :]

        def copy(self, kind, a):
            k = self.base + len(self.arrays) * self.KINDS.index(kind) + self.arrays.index(a)
            h = self.n // 2
            if kind in ('x0', 'x1', 'y0', 'y1'):
                lo = self.lo + h * int(kind[1])
                return remote(self.srcs[a].at[pl.ds(pl.multiple_of(lo, 16), h), :], self.blk(a, q_own, lo, h),
                              xnbr if kind[0] == 'x' else ynbr, k)
            if kind == 'yf':
                return remote(self.blk(a, q_x, self.lo, h), self.blk(a, q_x, self.lo, h), ynbr, k)
            if kind == 'xf':
                return remote(self.blk(a, q_y, self.lo + h, h), self.blk(a, q_y, self.lo + h, h), xnbr, k)
            q = {'x': q_x, 'y': q_y, 'd': q_d}[kind[1]]
            if kind[0] == 'z':
                b = self.blk(a, q, self.lo + h * int(kind[2]), h)
                return remote(b, b, znbr, k)
            return remote(self.blk(a, q, 0, SH), self.blk(a, q, 0, SH), partner, k)

        def start(self, *kinds):
            for kind in kinds:
                for a in self.arrays:
                    self.copy(kind, a).start()

        def recv(self, *kinds):
            for kind in kinds:
                for a in self.arrays:
                    self.copy(kind, a).wait_recv()

        def sent(self):
            for kind in self.KINDS[:15 if self.zsplit else 9]:
                for a in self.arrays:
                    self.copy(kind, a).wait_send()

    w_hbm = (w1_hbm, w3_hbm, w2_hbm)
    v_hbm = (v1_hbm, v3_hbm, v2_hbm)
    gw = Gather(0, w_hbm, w_v, (0, 1, 2), True)
    gva = Gather(45, v_hbm, v_out, (0,), True)
    gvb = Gather(60, v_hbm, v_out, (1, 2), False)

    def local(src, dst, k):
        return pltpu.make_async_copy(src, dst, lsem.at[k])

    pw = [remote(w_hbm[a], gw.blk(a, q_own, 0, SH), partner, 78 + a) for a in range(3)]
    pv = [remote(v_hbm[a], gva.blk(a, q_own, 0, SH), partner, 81 + a) for a in range(3)]
    lw = [local(w_hbm[a], gw.blk(a, q_own, 0, SH), a) for a in range(3)]
    lv = [local(v_hbm[a], gva.blk(a, q_own, 0, SH), 3 + a) for a in range(3)]

    def lx(i):
        cols = pl.ds(pl.multiple_of(i * TM, TM), TM)
        return [pltpu.make_async_copy(src.at[:, cols], dst.at[:, cols], xl.at[k, i])
                for k, (src, dst) in enumerate(((x_hbm, x_v), (dy_hbm, dy_v)))]

    def cols_of(q):
        return pl.ds(pl.multiple_of(q * CH, 128), CH)

    def unit(u):
        k = jnp.where(u < 9, u // 3, u - 9)
        m = jnp.where(u < 9, u % 3, 3)
        q = jnp.where(m == 0, q_d, jnp.where(m == 1, q_x, jnp.where(m == 2, q_y, q_own)))
        return k, 4 * k + m, cols_of(q)

    def half(h):
        return pl.ds(pl.multiple_of(h * HR, 16), HR)

    def g1_send(u):
        k, _, cq = unit(u)
        return rdma(g_hbm.at[k, half(1 - c), cq], r1.at[u], g1s.at[u], g1r.at[u], partner)

    def g2_loads(u):
        k, _, cq = unit(u)
        return (pltpu.make_async_copy(g_hbm.at[k, half(c), cq], gin2, g2l.at[0]),
                pltpu.make_async_copy(r1.at[u], rin, g2l.at[1]))

    def g2_out(u):
        _, km, _ = unit(u)
        return pltpu.make_async_copy(gout2, pp.at[km], g2l.at[2])

    def px(k, m):
        return rdma(pp.at[4 * k + m, pl.ds(0, QR), :], rx.at[k, m], gps.at[0, k, m], gpr.at[0, k, m], xnbr)

    def py(k, m):
        return rdma(pp.at[4 * k + 2 * m, pl.ds(QR, QR), :], ry.at[k, m], gps.at[1, k, m], gpr.at[1, k, m], ynbr)

    def g_sends(u):
        g2_out(u).wait()
        k = u // 3

        @pl.when((u < 9) & (u % 3 == 0))
        def _():
            px(k, 0).start()
            py(k, 0).start()

        @pl.when((u < 9) & (u % 3 == 1))
        def _():
            px(k, 1).start()

        @pl.when((u < 9) & (u % 3 == 2))
        def _():
            py(k, 1).start()

    def g_stage2(u):
        for cp in g2_loads(u):
            cp.wait()

        for r in range(0, HR, 48):
            gout2[r:r + 48, :] = (gin2[r:r + 48, :].astype(BF16).astype(F32) + rin[r:r + 48, :].astype(BF16).astype(F32)).astype(BF16)
        g2_out(u).start()

        @pl.when(u < 11)
        def _():
            g1_send(u + 1).wait_recv()
            for cp in g2_loads(u + 1):
                cp.start()

    def mid_sends(k):
        return (rdma(sy.at[k], ry2.at[k], gms.at[0, k], gmr.at[0, k], ynbr),
                rdma(sx.at[k], rx2.at[k], gms.at[1, k], gmr.at[1, k], xnbr))

    def ab_loads(k, fin):
        lo, hi = pl.ds(0, QR), pl.ds(QR, QR)
        if fin:
            srcs = (pp.at[4 * k + 3, lo, :], rx.at[k, 1], ry2.at[k], pp.at[4 * k + 3, hi, :], ry.at[k, 1], rx2.at[k])
        else:
            srcs = (pp.at[4 * k + 2, lo, :], rx.at[k, 0], pp.at[4 * k + 1, hi, :], ry.at[k, 0])
        return [pltpu.make_async_copy(s, ab.at[n], abl.at[n]) for n, s in enumerate(srcs)]

    def sg_half(s, k):
        return sg.at[s, k, half(c), :]

    def ob_outs(k, fin):
        if fin:
            dst = [sg.at[0, k, pl.ds(pl.multiple_of(c * HR + p * QR, 16), QR), :] for p in range(2)]
        else:
            dst = [sy.at[k], sx.at[k]]
        return [pltpu.make_async_copy(ob.at[p], dst[p], obs.at[p]) for p in range(2)]

    def z_sends(k):
        return (rdma(sg_half(0, k), sg_half(1, k), zs.at[0, k], zr.at[0, k], znbr),
                rdma(sg_half(0, k), sg_half(0, k), zs.at[1, k], zr.at[1, k], partner))

    def z_fwd(k):
        return rdma(sg_half(1, k), sg_half(1, k), zs.at[2, k], zr.at[2, k], partner)

    def g_load(k, fin):
        if fin:
            px(k, 1).wait_recv()
            py(k, 1).wait_recv()
            for cp in mid_sends(k):
                cp.wait_recv()
        else:
            px(k, 0).wait_recv()
            py(k, 0).wait_recv()
        for cp in ab_loads(k, fin):
            cp.start()

    def g_add(k, fin):
        for cp in ab_loads(k, fin):
            cp.wait()
        per = 3 if fin else 2

        def add(r, _):
            rows = pl.ds(pl.multiple_of(r * 48, 16), 48)
            for p in range(2):
                t = ab[per * p, rows, :].astype(F32)
                for e in range(1, per):
                    t = t + ab[per * p + e, rows, :].astype(F32)
                ob[p, rows, :] = t.astype(BF16)
            return 0
        lax.fori_loop(0, QR // 48, add, 0)
        for cp in ob_outs(k, fin):
            cp.start()

    def g_push(k, fin):
        for cp in ob_outs(k, fin):
            cp.wait()
        for cp in (z_sends(k) if fin else mid_sends(k)):
            cp.start()

    for cp in lw + lx(0):
        cp.start()
    bar = pltpu.get_barrier_semaphore()
    for dev in (partner, xnbr, ynbr, znbr):
        pl.semaphore_signal(bar, inc=1, device_id=dev, device_id_type=MESH)
    pl.semaphore_wait(bar, 4)
    for cp in pw:
        cp.start()
    gw.start('x0', 'y1', 'x1', 'y0')
    for i in range(1, NI):
        for cp in lx(i):
            cp.start()
    for cp in lw:
        cp.wait()
    for cp in pw:
        cp.wait_recv()

    def body(n, _):
        j = n // NI
        i = n % NI

        @pl.when(n <= S2 + 12)
        def _():
            @pl.when(n == 0)
            def _():
                for u in range(12):
                    g1_send(u).start()

            @pl.when(n == S2 - 1)
            def _():
                g1_send(0).wait_recv()
                for cp in g2_loads(0):
                    cp.start()

            @pl.when(n > S2)
            def _():
                g_sends(n - S2 - 1)

            @pl.when((n >= S2) & (n < S2 + 12))
            def _():
                g_stage2(n - S2)

        steps = {}

        def at(k):
            def put(f):
                steps.setdefault(k, []).append(f)
            return put

        @at(2)
        def _():
            gw.recv('x0')
            gw.start('zx0', 'yf')
            gw.recv('y1')
            gw.start('xf')

        @at(4)
        def _():
            gw.recv('x1')
            gw.start('zx1')
            gw.recv('y0')

        @at(5)
        def _():
            gw.start('zy1', 'zy0')
            for cp in lv + pv:
                cp.start()

        @at(6)
        def _():
            gva.start('x0', 'y1', 'x1', 'y0')

        @at(7)
        def _():
            gw.recv('zx0', 'zx1')
            gw.start('dx')

        @at(8)
        def _():
            gw.recv('dx')

        @at(10)
        def _():
            gw.recv('xf', 'yf')
            gw.start('zd0', 'zd1')

        @at(12)
        def _():
            gva.recv('x0')
            gva.start('yf', 'zx0')
            gva.recv('y1')
            gva.start('xf', 'zy1')
            gva.recv('x1')
            gva.start('zx1')
            gva.recv('y0')
            gva.start('zy0')

        @at(14)
        def _():
            gw.recv('zy0', 'zy1')
            gw.start('dy')

        @at(16)
        def _():
            gw.recv('dy')

        @at(17)
        def _():
            gva.recv('xf', 'yf')
            gva.start('zd0', 'zd1')

        @at(18)
        def _():
            gw.recv('zd0', 'zd1')
            gw.start('dd')

        @at(19)
        def _():
            gvb.start('x0', 'y1')

        @at(20)
        def _():
            gvb.start('x1', 'y0')

        @at(21)
        def _():
            gva.recv('zx0', 'zx1', 'zy0', 'zy1')
            gva.start('dx', 'dy')
            gva.recv('zd0', 'zd1')
            gva.start('dd')

        @at(24)
        def _():
            gw.recv('dd')
            z_sends(0)[0].wait_recv()
            z_fwd(0).start()

        @at(25)
        def _():
            gvb.recv('x0')
            gvb.start('yf')
            gvb.recv('y1')
            gvb.start('xf')

        @at(28)
        def _():
            z_sends(1)[0].wait_recv()
            z_fwd(1).start()

        @at(29)
        def _():
            gvb.recv('x1', 'y0')
            gvb.start('dx', 'dy')

        @at(30)
        def _():
            z_sends(2)[0].wait_recv()
            z_fwd(2).start()

        @at(31)
        def _():
            gvb.recv('xf', 'yf')
            gvb.start('dd')

        for e, (k, fin) in zip(G_AT, ((0, 0), (1, 0), (2, 0), (0, 1), (1, 1), (2, 1))):
            at(e + 2)(functools.partial(g_push, k, fin))
            at(e + 1)(functools.partial(g_add, k, fin))
            at(e)(functools.partial(g_load, k, fin))

        for jj in range(NC):
            @pl.when(j == jj)
            def _():
                for ii in range(NI):
                    if jj * NI + ii in steps:
                        @pl.when(i == ii)
                        def _():
                            for f in steps[jj * NI + ii]:
                                f()

        q = jnp.where(j == 0, q_own, jnp.where(j == 1, q_x, jnp.where(j == 2, q_y, q_d)))
        base = pl.multiple_of(q * CH, CH)

        @pl.when(i == 0)
        def _():
            def tr(r, _):
                src = pl.ds(pl.multiple_of(base + r * 128, 128), 128)
                for a in range(2):
                    wt[:, pl.ds(pl.multiple_of(a * CH + r * 128, 128), 128)] = w_v[a, src, :].T
                return 0
            lax.fori_loop(0, CH // 128, tr, 0)

        cols = pl.ds(pl.multiple_of(i * TM, TM), TM)
        slot = n % 2

        def hcopies(slot):
            return [pltpu.make_async_copy(hbuf.at[slot, pl.ds(a * CH, CH), :],
                                          h3_hbm.at[a, pl.ds(base, CH), cols], hsem.at[slot, a]) for a in range(2)]

        @pl.when(j == 0)
        def _():
            for cp in lx(i):
                cp.wait()

        dw_copy = pltpu.make_async_copy(dacc, dw_hbm.at[:, pl.ds(base, CH)], wsem)

        @pl.when((i == 0) & (j > 0))
        def _():
            dw_copy.wait()

        @pl.when(n >= 2)
        def _():
            for cp in hcopies(slot):
                cp.wait()

        for r in range(CH // SUB):
            src = pl.ds(pl.multiple_of(base + r * SUB, 16), SUB)
            a = dotf(w_v[0, src, :], x_v[:, cols], NN)
            b = dotf(w_v[1, src, :], x_v[:, cols], NN)
            dh = dotf(w_v[2, src, :], dy_v[:, cols], NN)
            s = 1.0 / (1.0 + jnp.exp(-a))
            act = a * s
            hbuf[slot, r * SUB:(r + 1) * SUB, :] = (dh * b * s * (1.0 + a * (1.0 - s))).astype(BF16)
            hbuf[slot, CH + r * SUB:CH + (r + 1) * SUB, :] = (dh * act).astype(BF16)
            h_v[r * SUB:(r + 1) * SUB, :] = (act * b).astype(BF16)
        for cp in hcopies(slot):
            cp.start()
        acc[:, cols] = jnp.where(j == 0, 0.0, acc[:, cols]) + dotf(wt[...], hbuf[slot], NN)
        dacc[...] = jnp.where(i == 0, 0.0, dacc[...]) + dotf(dy_v[:, cols], h_v[...], NT)

        @pl.when(i == NI - 1)
        def _():
            dw_copy.start()

        @pl.when(j == NC - 1)
        def _():
            x_v[:, cols] = acc[:, cols].astype(BF16)
            pltpu.make_async_copy(x_v.at[:, cols], dx_hbm.at[:, cols], xsem).start()
        return 0

    lax.fori_loop(0, NC * NI, body, 0)

    pltpu.make_async_copy(dacc, dw_hbm.at[:, pl.ds(0, CH)], wsem).wait()
    for slot in range(2):
        for a in range(2):
            pltpu.make_async_copy(hbuf.at[slot, pl.ds(a * CH, CH), :],
                                  h3_hbm.at[a, pl.ds(0, CH), pl.ds(0, TM)], hsem.at[slot, a]).wait()
    pltpu.make_async_copy(x_v, dx_hbm, xsem).wait()
    for cp in lv:
        cp.wait()
    for cp in pv:
        cp.wait_recv()
    for k in range(3):
        z_sends(k)[1].wait_recv()
        z_fwd(k).wait_recv()
    gvb.recv('dx', 'dy', 'dd')
    gva.recv('dx', 'dy', 'dd')
    for cp in pw + pv + [g1_send(u) for u in range(12)]:
        cp.wait_send()
    for g in (gw, gva, gvb):
        g.sent()
    for k in range(3):
        for m in range(2):
            px(k, m).wait_send()
            py(k, m).wait_send()
        for cp in mid_sends(k) + z_sends(k) + (z_fwd(k),):
            cp.wait_send()


def run_step(*args):
    hbm = pl.BlockSpec(memory_space=pltpu.MemorySpace.HBM)

    def out(*shape, dtype=BF16):
        return jax.ShapeDtypeStruct(shape, dtype)
    dma = pltpu.SemaphoreType.DMA
    return pl.pallas_call(
        step_kernel,
        out_shape=(out(2, F, T), out(D, F, dtype=F32), out(D, T), out(3, F, D), out(2, 3, D, CH),
                   out(12, HR, CH, dtype=F32), out(12, HR, CH), out(3, 2, QR, CH), out(3, 2, QR, CH),
                   out(3, QR, CH), out(3, QR, CH), out(3, QR, CH), out(3, QR, CH)),
        in_specs=[hbm] * 9,
        out_specs=(hbm,) * 13,
        scratch_shapes=[
            pltpu.VMEM((D, T), BF16), pltpu.VMEM((D, T), BF16), pltpu.VMEM((D, T), F32),
            pltpu.VMEM((3, F, D), BF16), pltpu.VMEM((D, 2 * CH), BF16),
            pltpu.VMEM((2, 2 * CH, TM), BF16), pltpu.VMEM((CH, TM), BF16), pltpu.VMEM((D, CH), F32),
            pltpu.VMEM((HR, CH), F32), pltpu.VMEM((HR, CH), F32), pltpu.VMEM((HR, CH), BF16),
            pltpu.VMEM((6, QR, CH), BF16), pltpu.VMEM((2, QR, CH), BF16),
            dma((6,)), dma((2, NI)), dma((2, 2)), dma, dma, dma((84,)), dma((84,)),
            dma((12,)), dma((12,)), dma((3,)), dma((2, 3, 2)), dma((2, 3, 2)),
            dma((6,)), dma((2,)), dma((2, 3)), dma((2, 3)), dma((3, 3)), dma((3, 3)),
        ],
        compiler_params=pltpu.CompilerParams(collective_id=0, has_side_effects=True,
                                             vmem_limit_bytes=66_900_000),
        cost_estimate=pl.CostEstimate(flops=12 * T * D * F, bytes_accessed=200_000_000, transcendentals=T * F),
    )(*args)


def grad_kernel(x_hbm, h3_ref, dwt_hbm, dx_hbm, v_ref, sg_ref,
                dw_hbm, dxo_hbm, v1o_ref, v3o_ref, v2o_ref, dn_ref,
                xs, ob, gt, tb, db, xsem, osem, isem, esem):
    s = pl.program_id(0)
    c = lax.axis_index('fsdp') % 2

    def out(s):
        return pltpu.make_async_copy(
            ob.at[s % 2], dw_hbm.at[0, s // 5, :, pl.ds(pl.multiple_of(s % 5 * 512, 512), 512)], osem.at[s % 2])

    def rows(s):
        return pl.ds(pl.multiple_of(s * RB, 16), RB)

    def ins(s):
        return (pltpu.make_async_copy(dwt_hbm.at[rows(s), :], tb.at[s % 2], isem.at[0, s % 2]),
                pltpu.make_async_copy(dx_hbm.at[rows(s), :], db.at[s % 2], isem.at[1, s % 2]))

    def outs(s):
        return (pltpu.make_async_copy(tb.at[s % 2], dw_hbm.at[0, 2, rows(s), :], esem.at[0, s % 2]),
                pltpu.make_async_copy(db.at[s % 2], dxo_hbm.at[rows(s), :], esem.at[1, s % 2]))

    def xq(k):
        return pltpu.make_async_copy(x_hbm.at[:, k * 1024:(k + 1) * 1024], xs.at[:, k * 1024:(k + 1) * 1024], xsem.at[k])

    def turn_v():
        for a, vo in enumerate((v1o_ref, v3o_ref, v2o_ref)):
            vo[...] = v_ref[a].T

    def turn_g():
        r = pl.ds(pl.multiple_of(s // 2 * 128, 128), 128)
        for k in range(3):
            gt[k, r, :] = (sg_ref[0, k].astype(F32) + sg_ref[1, k].astype(F32)).T

    @pl.when(s >= 2)
    def _():
        out(s - 2).wait()

    @pl.when(s == 0)
    def _():
        for k in range(4):
            xq(k).start()
        for cp in ins(0):
            cp.start()
        turn_g()
        turn_v()
        for k in range(4):
            xq(k).wait()
            kq = slice(k * 1024, (k + 1) * 1024)
            part = dotf(xs[:, kq], h3_ref[0, :, kq], NT)
            ob[0] = part if k == 0 else ob[0] + part

    @pl.when((s > 0) & (s % 2 == 0))
    def _():
        turn_g()
        turn_v()
        ob[0] = dotf(xs[...], h3_ref[0], NT)

    @pl.when(s % 2 == 1)
    def _():
        turn_v()
        ob[1] = dotf(xs[...], h3_ref[0], NT)

    out(s).start()
    for cp in ins(s):
        cp.wait()
    for cp in outs(s):
        cp.start()

    @pl.when(s > 0)
    def _():
        for cp in outs(s - 1):
            cp.wait()

    @pl.when(s < 9)
    def _():
        for cp in ins(s + 1):
            cp.start()

    @pl.when(s == 9)
    def _():
        dn_ref[...] = gt[:, pl.ds(pl.multiple_of(c * SH, 8), SH), :]
        out(8).wait()
        out(9).wait()
        for cp in outs(9):
            cp.wait()


def run_grad(x, h3, dwt, dx, v, sg):
    hbm = pl.BlockSpec(memory_space=pltpu.MemorySpace.HBM)
    vs = pl.BlockSpec((D, 256), lambda s: (0, s))
    dma = pltpu.SemaphoreType.DMA
    return pl.pallas_call(
        grad_kernel,
        grid=(10,),
        out_shape=(jax.ShapeDtypeStruct((1, 3, D, F), F32), jax.ShapeDtypeStruct((D, T), BF16),
                   jax.ShapeDtypeStruct((D, F), BF16), jax.ShapeDtypeStruct((D, F), BF16),
                   jax.ShapeDtypeStruct((D, F), BF16), jax.ShapeDtypeStruct((3, SH, D), F32)),
        in_specs=[hbm, pl.BlockSpec((1, 512, T), lambda s: (s // 5, s % 5, 0)), hbm, hbm,
                  pl.BlockSpec((3, 256, D), lambda s: (0, s, 0)),
                  pl.BlockSpec((2, 3, D, 128), lambda s: (0, 0, 0, s // 2))],
        out_specs=(hbm, hbm, vs, vs, vs,
                   pl.BlockSpec((3, SH, D), lambda s: (0, 0, 0), pipeline_mode=pl.Buffered(1))),
        scratch_shapes=[pltpu.VMEM((D, T), BF16), pltpu.VMEM((2, D, 512), F32), pltpu.VMEM((3, CH, D), F32),
                        pltpu.VMEM((2, RB, F), F32), pltpu.VMEM((2, RB, T), BF16),
                        dma((4,)), dma((2,)), dma((2, 2)), dma((2, 2))],
        compiler_params=pltpu.CompilerParams(vmem_limit_bytes=64_000_000),
        cost_estimate=pl.CostEstimate(flops=4 * T * D * F, bytes_accessed=150_000_000, transcendentals=0),
    )(x, h3, dwt, dx, v, sg)


def solution(mesh):
    def device_step(x, dy, w1, w3, w2, v1, v3, v2, g_next):
        xt, dyt = x.T, dy.T
        h3, dwt, dx, v, sg = run_step(xt, dyt, w1.T, w3.T, w2, v1.T, v3.T, v2, g_next[0])[:5]
        dw, dxo, v1o, v3o, v2o, dn = run_grad(xt, h3, dwt, dx, v, sg)
        return dxo.T, dn.transpose(0, 2, 1), dw, v1o, v3o, v2o.T

    row_spec = P(ALL_AXES, None)
    col_shard = P(None, FSDP_AXES)
    row_shard = P(FSDP_AXES, None)
    dev_spec = P(ALL_AXES, None, None, None)
    return jax.shard_map(
        device_step, mesh=mesh,
        in_specs=(row_spec, row_spec, col_shard, col_shard, row_shard, col_shard, col_shard, row_shard, dev_spec),
        out_specs=(row_spec, P(None, None, FSDP_AXES), dev_spec, P(), P(), P()),
        check_vma=False)
```
